512 devices in a mesh: gx: 32 (over y, x, core), gy: 16 (over z).
Axes of the slice: x: 4, y: 4, z: 16, core: 2. Of those that a mesh axis runs over, the one named last changes fastest.
Arguments:
- activations: bfloat16 [4096, 7168], P('gx', 'gy'), may hold values from -6 to 6
- out_grad: bfloat16 [4096, 7168], P('gx', 'gy'), may hold values from -0.59765625 to 0.59765625
- saved_gate: bfloat16 [4096, 8, 1024], P('gx', None, 'gy'), may hold values from -9 to 9
- saved_up: bfloat16 [4096, 8, 1024], P('gx', None, 'gy'), may hold values from -6 to 6
- route_ids: int32 [4096, 8], P('gx'), may hold values from 0 to 31, all different within a row; in each aligned block of 128 rows (0 to 127, 128 to 255, ...) at most 48 rows name the same one
- route_weight: float32 [4096, 8], P('gx'), may hold values from 0.1 to 1
- down_weight: bfloat16 [32, 1024, 7168], P('gx', None, 'gy'), may hold values from -0.1875 to 0.1875
Outputs:
- grad_gate: bfloat16 [32, 7168, 1024], P('gx', 'gy')
- grad_up: bfloat16 [32, 7168, 1024], P('gx', 'gy')
- grad_down: bfloat16 [32, 1024, 7168], P('gx', None, 'gy')
The draws below stay inside these ranges and needn't reach their ends.
Inputs may be any that keep to these rules, and one draw needn't show every extreme that they name: `route_ids`: each token names 8 different experts. Within each aligned block of 128 tokens (one index of gx) no expert is named by more than 48 tokens, a bound that some block reaches.
All inputs are finite; a program needn't handle non-finite values.
Results may differ from the reference program's by a relative error of at most 0.02.
Values may be sent and summed in bfloat16 or wider, within the bound.
No kernel may reach another device: no remote copies, remote signals or barrier semaphores. Data moves between devices by JAX's collectives and lax.ppermute only.
A program may use at most 64 MiB of HBM per device.

```python
import math
import jax
import jax.numpy as jnp
import numpy as np
from jax import lax

D = 7168
HIDDEN_SIZE = 1024
TOK_DEV = 128
TOP = 8
MOST = 48
EXPERTS = 32
TOKENS = 4096
ROWS = 1536
N_GX = 32
N_GY = 16


def level_of(key, shape, pieces, smallest, high):
    level, own = 1.0, jax.random.fold_in(key, 6)
    for position, blocks in pieces:
        heights = jnp.exp(jax.random.uniform(jax.random.fold_in(own, position), (blocks,), jnp.float32, smallest / len(pieces), high / len(pieces)))
        level = level * jnp.repeat(heights, shape[position] // blocks).reshape([-1 if axis == position else 1 for axis in range(len(shape))])
    return level


def assign_block(key, own, number, rows, number_of, top, most, lean):
    ranking = jax.random.permutation(key, number_of)
    crowded, ordinary = portions_of(number_of, rows * top, most, lean, True), portions_of(number_of, rows * top, most, lean, False)
    places = jnp.arange(number_of)

    def named(tallies, rotation):
        used = int((tallies > 0).sum())
        fixed = max(1, used // 4)
        moved = fixed + (places - fixed + rotation * (used - fixed)) % max(1, number_of - fixed)
        return jnp.zeros((number_of,), jnp.int32).at[ranking[jnp.where(places < fixed, places, moved)]].set(jnp.asarray(tallies, jnp.int32))

    tallies = jnp.where(number % 4 == 0, named(crowded, number // 4), named(ordinary, number - number // 4 - 1))
    mixed = jax.random.permutation(jax.random.fold_in(own, 3), number_of)
    donor, sink = mixed[0:number_of // 2 * 2:2], mixed[1:number_of // 2 * 2:2]
    slack = jnp.minimum(tallies[donor] - 1, most - tallies[sink]) // 2
    slack = jnp.where((donor == ranking[0]) | (sink == ranking[0]) | (tallies[sink] == 0), 0, jnp.maximum(slack, 0))
    moved = jax.random.randint(jax.random.fold_in(own, 4), (number_of // 2,), 0, 1 << 20) % (slack + 1)
    tallies = tallies.at[donor].add(-moved).at[sink].add(moved)
    items = jnp.searchsorted(jnp.cumsum(tallies), jnp.arange(rows * top), side="right").astype(jnp.int32)
    grid = items.reshape(top, rows).T
    grid = grid[jax.random.permutation(jax.random.fold_in(own, 1), rows)]
    rotation = jax.random.randint(jax.random.fold_in(own, 2), (rows, 1), 0, top)
    return jnp.take_along_axis(grid, (jnp.arange(top)[None, :] + rotation) % top, axis=1)


def portions_of(number_of, total, limit, skew, full):
    loads = [(1 << 20) // math.isqrt(standing ** skew) + 1 for standing in range(1, number_of + 1)]
    largest = limit if full else min(limit, max(-(-total // number_of), total * loads[0] // sum(loads)))
    least = 1 if total - largest >= number_of - 1 else 0
    holding, rest = [largest] + [least] * (number_of - 1), total - largest - least * (number_of - 1)
    while rest > 0:
        candidates = [i for i in range(1, number_of) if holding[i] < largest] or [i for i in range(1, number_of) if holding[i] < limit]
        whole, left = sum([loads[i] for i in candidates]), rest
        for i in candidates:
            extra = min(limit - holding[i], max(1, left * loads[i] // whole), rest)
            holding[i] = holding[i] + extra
            rest = rest - extra
    return np.array(holding)


def normal_values(rng, shape, spread, bound, pieces=(), kind=jnp.bfloat16):
    values = spread * jax.random.normal(rng, shape, jnp.float32)
    if pieces:
        values = values * level_of(rng, shape, pieces, -0.22, 0.18)
    return jnp.clip(values, -bound, bound).astype(kind)


def setup_inputs(seed: int = 0) -> dict:
    streams_of = jax.random.split(jax.random.key(seed), 8)
    activations = normal_values(streams_of[0], (TOKENS, D), 1.0, 6.0, ((0, 32), (1, 16)))
    out_grad = normal_values(streams_of[1], (TOKENS, D), 0.1, 0.59765625, ((0, 32), (1, 16)))
    saved_gate = normal_values(streams_of[2], (TOKENS, TOP, HIDDEN_SIZE), 1.5, 9.0, ((0, 32), (2, 16)))
    saved_up = normal_values(streams_of[3], (TOKENS, TOP, HIDDEN_SIZE), 1.0, 6.0, ((0, 32), (2, 16)))
    route_ids_keys = jax.random.split(jax.random.fold_in(streams_of[4], 1), TOKENS // TOK_DEV)
    route_ids_turns = jax.random.permutation(jax.random.fold_in(streams_of[4], 3), TOKENS // TOK_DEV)
    route_ids = jax.vmap(lambda own, number: assign_block(jax.random.fold_in(streams_of[4], 2), own, number, TOK_DEV, EXPERTS, TOP, MOST, 2))(route_ids_keys, route_ids_turns).reshape((TOKENS, TOP))
    route_weight = jnp.clip(jnp.exp(math.log(1.0) - 2.3025851 * jax.random.uniform(streams_of[5], (TOKENS, TOP), jnp.float32) ** level_of(streams_of[5], (TOKENS, TOP), ((0, 32),), -0.2, 0.2)), 0.1, 1.0)
    down_weight = normal_values(streams_of[6], (EXPERTS, HIDDEN_SIZE, D), HIDDEN_SIZE ** -0.5, 0.1875, ((0, 32), (2, 16)))
    return {"activations": activations, "out_grad": out_grad, "saved_gate": saved_gate, "saved_up": saved_up, "route_ids": route_ids, "route_weight": route_weight, "down_weight": down_weight}


def local_grads(hidden_grad, gate_rows, up_rows):
    gate_val = gate_rows.astype(jnp.float32)
    up_val = up_rows.astype(jnp.float32)
    gate_sig = jax.nn.sigmoid(gate_val)
    silu_val = gate_val * gate_sig
    hidden_act = (silu_val * up_val).astype(jnp.bfloat16)
    grad_upper = (hidden_grad * silu_val).astype(jnp.bfloat16)
    grad_gated = (hidden_grad * up_val * gate_sig * (1.0 + gate_val * (1.0 - gate_sig))).astype(jnp.bfloat16)
    return hidden_act, grad_gated, grad_upper


def contract_rows(left, right):
    return lax.dot_general(left, right, (((0,), (0,)), ((), ())), preferred_element_type=jnp.float32).astype(jnp.bfloat16)


def reference(activations, out_grad, saved_gate, saved_up, route_ids, route_weight, down_weight):
    routes_all = TOKENS * TOP
    block_ids = route_ids.reshape(N_GX, TOK_DEV * TOP)
    onehot = (block_ids[:, :, None] == jnp.arange(EXPERTS, dtype=jnp.int32)[None, None, :]).astype(jnp.int32)
    rank_in = jnp.sum((jnp.cumsum(onehot, axis=1) - onehot) * onehot, axis=2).reshape(-1).astype(jnp.int32)
    source = (jnp.arange(routes_all, dtype=jnp.int32) // (TOK_DEV * TOP)).astype(jnp.int32)
    flat_ids = route_ids.reshape(-1).astype(jnp.int32)
    destination = (flat_ids * ROWS + source * MOST + rank_in).astype(jnp.int32)
    numbers = jnp.arange(routes_all, dtype=jnp.int32) + 1
    row_table = jnp.zeros((EXPERTS * ROWS,), jnp.int32).at[destination].set(numbers).reshape(EXPERTS, ROWS)
    flat_weight = route_weight.reshape(-1)
    gate_flat = saved_gate.reshape(routes_all, HIDDEN_SIZE)
    up_flat = saved_up.reshape(routes_all, HIDDEN_SIZE)
    nothing = jnp.zeros((), jnp.bfloat16)

    def one_expert(packed):
        entry, weight = packed
        is_live = (entry > 0)[:, None]
        route_at = jnp.maximum(entry - 1, 0).astype(jnp.int32)
        token_at = (route_at // TOP).astype(jnp.int32)
        rows_act = jnp.where(is_live, activations[token_at], nothing)
        scaled = (flat_weight[route_at][:, None] * out_grad[token_at].astype(jnp.float32)).astype(jnp.bfloat16)
        rows_grad = jnp.where(is_live, scaled, nothing)
        gate_rows = jnp.where(is_live, gate_flat[route_at], nothing)
        up_rows = jnp.where(is_live, up_flat[route_at], nothing)
        split_grad = rows_grad.reshape(ROWS, N_GY, D // N_GY).astype(jnp.float32)
        split_weight = weight.reshape(HIDDEN_SIZE, N_GY, D // N_GY).astype(jnp.float32)
        partial_value = jnp.einsum("rgd,fgd->grf", split_grad, split_weight).astype(jnp.bfloat16)
        partial_value = lax.optimization_barrier(partial_value)
        hidden_grad = jnp.sum(partial_value.astype(jnp.float32), axis=0)
        hidden_act, grad_gated, grad_upper = local_grads(hidden_grad, gate_rows, up_rows)
        return contract_rows(rows_act, grad_gated), contract_rows(rows_act, grad_upper), contract_rows(hidden_act, rows_grad)

    grad_gate, grad_up, grad_down = lax.map(one_expert, (row_table, down_weight))
    return grad_gate, grad_up, grad_down
```

```python
import jax
import jax.numpy as jnp
from jax import lax
from jax.experimental import pallas as pl
from jax.experimental.pallas import tpu as pltpu
from jax.sharding import Mesh
from jax.sharding import PartitionSpec as P

MOST = 48
GX = ("gx_0", "gx_1", "gx_2")
F32 = jnp.float32
BF16 = jnp.bfloat16


def nt_dot(left, right):
    return lax.dot_general(left, right, (((1,), (1,)), ((), ())), preferred_element_type=F32)


def vmem_call(kernel, out_shapes, flops, size, scratch=()):
    return pl.pallas_call(
        kernel,
        out_shape=out_shapes,
        scratch_shapes=scratch,
        cost_estimate=pl.CostEstimate(flops=flops, bytes_accessed=size, transcendentals=0),
        compiler_params=pltpu.CompilerParams(vmem_limit_bytes=40 * 2**20),
    )


def pack_kernel(ids_ref, weight_ref, gate_ref, up_ref, grad_ref, gu_out, rows_out, place_out, key_ref, share_ref):
    experts, tokens = key_ref.shape
    tops = ids_ref.shape[0]
    expert_at = lax.broadcasted_iota(jnp.int32, (experts, tokens), 0)
    named = jnp.zeros((experts, tokens), F32)
    share = jnp.zeros((experts, tokens), F32)
    for k in range(tops):
        hit = ids_ref[pl.ds(k, 1), :] == expert_at
        named = named + jnp.where(hit, 1.0, 0.0)
        share = share + jnp.where(hit, weight_ref[pl.ds(k, 1), :], 0.0)
    before = (
        lax.broadcasted_iota(jnp.int32, (tokens, tokens), 0)
        < lax.broadcasted_iota(jnp.int32, (tokens, tokens), 1)
    ).astype(F32)
    earlier = jnp.dot(named.astype(BF16), before.astype(BF16), preferred_element_type=F32)
    key_ref[...] = jnp.where(named > 0.5, earlier.astype(jnp.int32), -1)
    share_ref[...] = share
    rank = lax.broadcasted_iota(jnp.int32, (MOST, tokens), 0)
    group = 4

    def step(at, carry):
        places, scales, chosen = [], [], [[] for _ in range(tops)]
        for i in range(group):
            e = at * group + i
            mine = key_ref[pl.ds(e, 1), :] == rank
            places.append(jnp.where(mine, 1.0, 0.0))
            scales.append(jnp.sum(jnp.where(mine, share_ref[pl.ds(e, 1), :], 0.0), axis=1, keepdims=True))
            for k in range(tops):
                wanted = jnp.where(ids_ref[pl.ds(k, 1), :] == e, 1.0, 0.0)
                chosen[k].append(places[-1] * wanted)
        place = jnp.concatenate(places, axis=0).astype(BF16)
        scale = jnp.concatenate(scales, axis=0)
        gate = jnp.zeros((group * MOST, gate_ref.shape[1]), F32)
        up = jnp.zeros((group * MOST, gate_ref.shape[1]), F32)
        for k in range(tops):
            pick = jnp.concatenate(chosen[k], axis=0).astype(BF16)
            gate = gate + nt_dot(pick, gate_ref[k])
            up = up + nt_dot(pick, up_ref[k])
        rows = pl.ds(pl.multiple_of(at * (group * MOST), group * MOST), group * MOST)
        gu_out[rows, :] = jnp.concatenate([gate, up], axis=1).astype(BF16)
        rows_out[rows, :] = (nt_dot(place, grad_ref[...]) * scale).astype(BF16)
        place_out[rows, :] = place
        return carry

    lax.fori_loop(0, experts // group, step, 0)


def place_kernel(place_ref, values_ref, after_ref, out_ref):
    out_ref[...] = nt_dot(place_ref[...], values_ref[...]).astype(BF16)


def turn_kernel(rows_ref, out_ref):
    out_ref[...] = rows_ref[...].astype(F32).T.astype(BF16)


def gates_kernel(both_ref, after_ref, act_ref, upper_ref, gated_ref):
    half = act_ref.shape[0]
    gate = both_ref[0, :half, :].astype(F32)
    up = both_ref[0, half:, :].astype(F32)
    sig = 1.0 / (1.0 + jnp.exp(-gate))
    silu = gate * sig
    act_ref[...] = (silu * up).astype(BF16)
    upper_ref[...] = silu
    gated_ref[...] = up * sig * (1.0 + gate * (1.0 - sig))


def gates(both, after):
    count, width, rows = both.shape
    half = width // 2
    spec = pl.BlockSpec((half, rows), lambda i: (i, 0))
    return pl.pallas_call(
        gates_kernel,
        grid=(count,),
        in_specs=[
            pl.BlockSpec((1, width, rows), lambda i: (i, 0, 0)),
            pl.BlockSpec(memory_space=pl.ANY),
        ],
        out_specs=[spec, spec, spec],
        out_shape=[
            jax.ShapeDtypeStruct((count * half, rows), BF16),
            jax.ShapeDtypeStruct((count * half, rows), F32),
            jax.ShapeDtypeStruct((count * half, rows), F32),
        ],
        cost_estimate=pl.CostEstimate(flops=20 * count * half * rows, bytes_accessed=14 * count * half * rows, transcendentals=count * half * rows),
    )(both, after)


def ring_sum(chunks, axis):
    count = len(chunks)
    plus = [(i, (i + 1) % count) for i in range(count)]
    minus = [(i, (i - 1) % count) for i in range(count)]
    far = count // 2

    def add(moving, own):
        return (moving.astype(F32) + own.astype(F32)).astype(BF16)

    ahead, behind = (chunks[far], chunks[far + 1])
    for s in range(far):
        ahead = lax.ppermute(ahead, axis, plus)
        if s < far - 1:
            behind = lax.ppermute(behind, axis, minus)
        if s < far - 1:
            ahead = add(ahead, chunks[far - 1 - s])
        if s < far - 2:
            behind = add(behind, chunks[far + 2 + s])
    return (ahead.astype(F32) + behind.astype(F32) + chunks[0].astype(F32)).astype(BF16)


def on_device(activations, out_grad, saved_gate, saved_up, route_ids, route_weight, down_weight):
    experts = lax.axis_size(GX)
    planes = lax.axis_size("gy")
    z = lax.axis_index("gy")
    tokens, width = activations.shape
    slots = experts * MOST
    share = saved_gate.shape[2]
    hidden = down_weight.shape[1]
    sds = jax.ShapeDtypeStruct
    gu_routes, grad_routes, place = vmem_call(
        pack_kernel,
        [sds((slots, 2 * share), BF16), sds((slots, width), BF16), sds((slots, tokens), BF16)],
        2 * slots * tokens * (width + 16 * share),
        4 * slots * width,
        [pltpu.VMEM((experts, tokens), jnp.int32), pltpu.VMEM((experts, tokens), F32)],
    )(
        route_ids.T,
        route_weight.T,
        jnp.transpose(saved_gate, (1, 2, 0)),
        jnp.transpose(saved_up, (1, 2, 0)),
        out_grad.T,
    )
    gu_rows = lax.all_to_all(gu_routes.reshape(experts, MOST, -1), GX, 0, 0, tiled=True)
    gu_share = vmem_call(turn_kernel, sds((2 * share, slots), BF16), 0, 8 * slots * share)(
        gu_rows.reshape(slots, 2 * share)
    )
    gu_all = lax.all_gather(gu_share, "gy", axis=0)
    rows_grad = lax.all_to_all(grad_routes.reshape(experts, MOST, -1), GX, 0, 0, tiled=True)
    rows_grad = rows_grad.reshape(slots, width)
    weight = down_weight[0]
    turned = lax.dynamic_slice(jnp.concatenate([weight, weight], axis=0), (z * share, 0), weight.shape)
    partial = nt_dot(turned, rows_grad).astype(BF16)
    chunks = [partial[share * j : share * (j + 1)] for j in range(planes)]
    hidden_share = ring_sum(chunks, "gy")
    hidden_grad = lax.all_gather(hidden_share, "gy", axis=0, tiled=True)
    act_routes = vmem_call(
        place_kernel, sds((slots, width), BF16), 2 * slots * tokens * width, 2 * slots * width
    )(place, activations.T, hidden_share)
    rows_act = lax.all_to_all(act_routes.reshape(experts, MOST, -1), GX, 0, 0, tiled=True)
    rows_act = rows_act.reshape(slots, width)
    hidden_act, upper_by, gated_by = gates(gu_all, hidden_share)
    down_t = lax.dot_general(rows_grad, hidden_act, (((0,), (1,)), ((), ())), preferred_element_type=F32)
    hidden_grad = hidden_grad.astype(F32)
    gated = (hidden_grad * gated_by).astype(BF16)
    upper = (hidden_grad * upper_by).astype(BF16)

    def by_rows(values):
        return lax.dot_general(
            rows_act, values, (((0,), (1,)), ((), ())), preferred_element_type=F32
        ).astype(BF16)[None]

    return (by_rows(gated), by_rows(upper), down_t.astype(BF16).T[None])


def solution(mesh):
    torus = Mesh(mesh.devices.reshape(4, 4, 2, mesh.shape["gy"]), ("gx_0", "gx_1", "gx_2", "gy"))
    return jax.shard_map(
        on_device,
        mesh=torus,
        in_specs=(
            P(GX, "gy"),
            P(GX, "gy"),
            P(GX, None, "gy"),
            P(GX, None, "gy"),
            P(GX, None),
            P(GX, None),
            P(GX, None, "gy"),
        ),
        out_specs=(P(GX, "gy", None), P(GX, "gy", None), P(GX, None, "gy")),
        check_vma=False,
    )
```

```python
import jax
import jax.numpy as jnp
from jax import lax
from jax.experimental import pallas as pl
from jax.experimental.pallas import tpu as pltpu
from jax.sharding import Mesh
from jax.sharding import PartitionSpec as P

MOST = 48
GX = ("gx_0", "gx_1", "gx_2")
F32 = jnp.float32
BF16 = jnp.bfloat16


def nt_dot(left, right):
    return lax.dot_general(left, right, (((1,), (1,)), ((), ())), preferred_element_type=F32)


def vmem_call(kernel, out_shapes, flops, size, scratch=()):
    return pl.pallas_call(
        kernel,
        out_shape=out_shapes,
        scratch_shapes=scratch,
        cost_estimate=pl.CostEstimate(flops=flops, bytes_accessed=size, transcendentals=0),
        compiler_params=pltpu.CompilerParams(vmem_limit_bytes=16 * 2**20),
    )


def pack_kernel(
    ids_hbm, weight_hbm, gate_hbm, up_hbm, grad_hbm, rows_out, place_out,
    ids_ref, weight_ref, gate_ref, up_ref, grad_ref, both_ref, key_ref, share_ref, sems,
):
    pairs = (
        (ids_hbm, ids_ref),
        (weight_hbm, weight_ref),
        (gate_hbm, gate_ref),
        (up_hbm, up_ref),
        (grad_hbm, grad_ref),
    )
    copies = [pltpu.make_async_copy(src, dst, sems.at[i]) for i, (src, dst) in enumerate(pairs)]
    for copy in copies:
        copy.start()
    experts, tokens = key_ref.shape
    tops = ids_ref.shape[0]
    half = gate_ref.shape[1]
    expert_at = lax.broadcasted_iota(jnp.int32, (experts, tokens), 0)
    named = jnp.zeros((experts, tokens), F32)
    share = jnp.zeros((experts, tokens), F32)
    copies[0].wait()
    copies[1].wait()
    for k in range(tops):
        hit = ids_ref[pl.ds(k, 1), :] == expert_at
        named = named + jnp.where(hit, 1.0, 0.0)
        share = share + jnp.where(hit, weight_ref[pl.ds(k, 1), :], 0.0)
    before = (
        lax.broadcasted_iota(jnp.int32, (tokens, tokens), 0)
        < lax.broadcasted_iota(jnp.int32, (tokens, tokens), 1)
    ).astype(F32)
    earlier = jnp.dot(named.astype(BF16), before.astype(BF16), preferred_element_type=F32)
    key_ref[...] = jnp.where(named > 0.5, earlier.astype(jnp.int32), -1)
    share_ref[...] = share
    copies[2].wait()
    copies[3].wait()
    for k in range(tops):
        both_ref[:half, tokens * k : tokens * (k + 1)] = gate_ref[k]
        both_ref[half:, tokens * k : tokens * (k + 1)] = up_ref[k]
    copies[4].wait()
    rank = lax.broadcasted_iota(jnp.int32, (MOST, tokens), 0)
    group = 4

    def step(at, carry):
        places, scales, chosen = [], [], []
        for i in range(group):
            e = at * group + i
            mine = key_ref[pl.ds(e, 1), :] == rank
            places.append(jnp.where(mine, 1.0, 0.0))
            scales.append(jnp.sum(jnp.where(mine, share_ref[pl.ds(e, 1), :], 0.0), axis=1, keepdims=True))
            chosen.append(
                jnp.concatenate(
                    [
                        places[-1] * jnp.where(ids_ref[pl.ds(k, 1), :] == e, 1.0, 0.0)
                        for k in range(tops)
                    ],
                    axis=1,
                )
            )
        place = jnp.concatenate(places, axis=0).astype(BF16)
        scale = jnp.concatenate(scales, axis=0)
        pick = jnp.concatenate(chosen, axis=0).astype(BF16)
        rows = pl.ds(pl.multiple_of(at * (group * MOST), group * MOST), group * MOST)
        rows_out[rows, : 2 * half] = nt_dot(pick, both_ref[...]).astype(BF16)
        rows_out[rows, 2 * half :] = (nt_dot(place, grad_ref[...]) * scale).astype(BF16)
        place_out[rows, :] = place
        return carry

    lax.fori_loop(0, experts // group, step, 0)


def place_kernel(place_ref, values_ref, after_ref, out_ref):
    out_ref[...] = nt_dot(place_ref[...], values_ref[...]).astype(BF16)


def turn_kernel(rows_ref, out_ref):
    out_ref[...] = rows_ref[...].astype(F32).T.astype(BF16)


def weight_kernel(at_ref, weight_ref, ahead_ref, behind_ref, turned_ref):
    turned_ref[...] = weight_ref[...].astype(F32).T.astype(BF16)
    z = at_ref[0]
    near, far = (ahead_ref.shape[0], behind_ref.shape[0])
    share = (near - far) // 2
    planes = (near + far) // share
    for j in range(planes):
        start = pl.multiple_of(lax.rem(z + j, planes) * share, share)
        chunk = turned_ref[pl.ds(start, share), :]
        if j * share < near:
            ahead_ref[j * share : (j + 1) * share, :] = chunk
        else:
            behind_ref[j * share - near : (j + 1) * share - near, :] = chunk


def unpack_kernel(rows_ref, grad_ref, act_ref, upper_ref, gated_ref):
    half = act_ref.shape[0]
    grad_ref[...] = rows_ref[:, 2 * half :]
    both = rows_ref[:, : 2 * half].astype(F32).T
    gate = both[:half]
    up = both[half:]
    sig = 1.0 / (1.0 + jnp.exp(-gate))
    silu = gate * sig
    act_ref[...] = (silu * up).astype(BF16)
    upper_ref[...] = silu
    gated_ref[...] = up * sig * (1.0 + gate * (1.0 - sig))


def scale_kernel(ahead_ref, behind_ref, own_ref, upper_ref, gated_ref, first_ref, second_ref):
    half = ahead_ref.shape[0]
    split = first_ref.shape[1]
    total = ahead_ref[...].astype(F32) + behind_ref[...].astype(F32) + own_ref[...].astype(F32)
    gated = (total * gated_ref[...]).astype(BF16)
    upper = (total * upper_ref[...]).astype(BF16)
    first_ref[:half, :] = gated[:, :split]
    first_ref[half:, :] = upper[:, :split]
    second_ref[:half, :] = gated[:, split:]
    second_ref[half:, :] = upper[:, split:]


def final_kernel(at_ref, act_ref, first_ref, second_ref, gate_out, up_out):
    count, both, split = first_ref.shape
    planes = second_ref.shape[0]
    half = both // 2
    base = pl.program_id(0) * count + planes - at_ref[0]
    for out, low in ((gate_out, 0), (up_out, half)):
        head = first_ref[:, low : low + half, :].reshape(count * half, split)
        tail = jnp.concatenate(
            [second_ref[lax.rem(base + i, planes), low : low + half, :] for i in range(count)], axis=0
        )
        out[...] = (nt_dot(act_ref[:, :split], head) + nt_dot(act_ref[:, split:], tail)).astype(BF16)


def final_grads(at, act_turned, first, second):
    width, slots = act_turned.shape
    planes, both, split = first.shape
    group = 4
    wide = group * both // 2
    spec = pl.BlockSpec((width, wide), lambda i: (0, i))
    shape = jax.ShapeDtypeStruct((width, planes * both // 2), BF16)
    return pl.pallas_call(
        final_kernel,
        grid=(planes // group,),
        in_specs=[
            pl.BlockSpec(memory_space=pltpu.SMEM),
            pl.BlockSpec((width, slots), lambda i: (0, 0)),
            pl.BlockSpec((group, both, split), lambda i: (i, 0, 0)),
            pl.BlockSpec((planes, both, slots - split), lambda i: (0, 0, 0)),
        ],
        out_specs=[spec, spec],
        out_shape=[shape, shape],
        cost_estimate=pl.CostEstimate(
            flops=2 * width * slots * planes * both, bytes_accessed=2 * slots * planes * both, transcendentals=0
        ),
        compiler_params=pltpu.CompilerParams(vmem_limit_bytes=16 * 2**20),
    )(at, act_turned, first, second)


def add(moving, own):
    return (moving.astype(F32) + own.astype(F32)).astype(BF16)


def ring_pairs(count):
    return (
        [(i, (i + 1) % count) for i in range(count)],
        [(i, (i - 1) % count) for i in range(count)],
    )


def ring_sums(near, past, axis):
    far = len(near) - 1
    plus, minus = ring_pairs(len(near) + len(past))
    ahead, behind = (near[far], past[0])
    for s in range(far):
        ahead = lax.ppermute(ahead, axis, plus)
        if s < far - 1:
            behind = lax.ppermute(behind, axis, minus)
            ahead = add(ahead, near[far - 1 - s])
        if s < far - 2:
            behind = add(behind, past[1 + s])
    return ahead, behind


def ring_gather(share, axis, count):
    plus, minus = ring_pairs(count)
    whole = jnp.zeros((count, *share.shape), share.dtype).at[0].set(share)
    ahead = behind = share
    for s in range(count // 2):
        ahead = lax.ppermute(ahead, axis, plus)
        whole = whole.at[count - 1 - s].set(ahead)
        if s < count // 2 - 1:
            behind = lax.ppermute(behind, axis, minus)
            whole = whole.at[1 + s].set(behind)
    return whole


def on_device(activations, out_grad, saved_gate, saved_up, route_ids, route_weight, down_weight):
    experts = lax.axis_size(GX)
    planes = lax.axis_size("gy")
    z = lax.axis_index("gy")
    tokens, width = activations.shape
    tops = route_ids.shape[1]
    slots = experts * MOST
    half = saved_gate.shape[2]
    hidden = down_weight.shape[1]
    split = slots * 2 // 3
    sds = jax.ShapeDtypeStruct
    hbm = pl.BlockSpec(memory_space=pltpu.MemorySpace.HBM)
    routes, place = pl.pallas_call(
        pack_kernel,
        in_specs=[hbm] * 5,
        out_shape=[sds((slots, 2 * half + width), BF16), sds((slots, tokens), BF16)],
        scratch_shapes=[
            pltpu.VMEM((tops, tokens), jnp.int32),
            pltpu.VMEM((tops, tokens), F32),
            pltpu.VMEM((tops, half, tokens), BF16),
            pltpu.VMEM((tops, half, tokens), BF16),
            pltpu.VMEM((width, tokens), BF16),
            pltpu.VMEM((2 * half, tops * tokens), BF16),
            pltpu.VMEM((experts, tokens), jnp.int32),
            pltpu.VMEM((experts, tokens), F32),
            pltpu.SemaphoreType.DMA((5,)),
        ],
        cost_estimate=pl.CostEstimate(
            flops=2 * slots * tokens * (width + 16 * half), bytes_accessed=4 * slots * width, transcendentals=0
        ),
        compiler_params=pltpu.CompilerParams(vmem_limit_bytes=16 * 2**20),
    )(
        route_ids.T,
        route_weight.T,
        jnp.transpose(saved_gate, (1, 2, 0)),
        jnp.transpose(saved_up, (1, 2, 0)),
        out_grad.T,
    )
    near = (planes // 2 + 1) * half
    ahead_weight, behind_weight = pl.pallas_call(
        weight_kernel,
        in_specs=[pl.BlockSpec(memory_space=pltpu.SMEM), pl.BlockSpec(memory_space=pltpu.VMEM)],
        out_shape=[sds((near, width), BF16), sds((hidden - near, width), BF16)],
        scratch_shapes=[pltpu.VMEM((hidden, width), BF16)],
        cost_estimate=pl.CostEstimate(flops=0, bytes_accessed=6 * hidden * width, transcendentals=0),
        compiler_params=pltpu.CompilerParams(vmem_limit_bytes=16 * 2**20),
    )(z.reshape(1), down_weight[0].T)
    rows = lax.all_to_all(routes.reshape(experts, MOST, -1), GX, 0, 0, tiled=True).reshape(slots, -1)
    rows_grad, act_share, upper_by, gated_by = vmem_call(
        unpack_kernel,
        [sds((slots, width), BF16), sds((half, slots), BF16), sds((half, slots), F32), sds((half, slots), F32)],
        20 * half * slots,
        4 * slots * width,
    )(rows)
    hidden_act = lax.all_gather(act_share, "gy", axis=0, tiled=True)
    near_sums = nt_dot(ahead_weight, rows_grad).astype(BF16)
    past_sums = nt_dot(behind_weight, rows_grad).astype(BF16)
    near_chunks = [near_sums[half * j : half * (j + 1)] for j in range(planes // 2 + 1)]
    past_chunks = [past_sums[half * j : half * (j + 1)] for j in range(planes // 2 - 1)]
    ahead, behind = ring_sums(near_chunks, past_chunks, "gy")
    first, second = vmem_call(
        scale_kernel,
        [sds((2 * half, split), BF16), sds((2 * half, slots - split), BF16)],
        4 * half * slots,
        20 * half * slots,
    )(ahead, behind, near_chunks[0], upper_by, gated_by)
    first = lax.all_gather(first, "gy", axis=0)
    act_routes = vmem_call(
        place_kernel, sds((slots, width), BF16), 2 * slots * tokens * width, 2 * slots * width
    )(place, activations.T, second)
    rows_act = lax.all_to_all(act_routes.reshape(experts, MOST, -1), GX, 0, 0, tiled=True)
    second = ring_gather(second, "gy", planes)
    act_turned = vmem_call(turn_kernel, sds((width, slots), BF16), 0, 4 * slots * width)(
        rows_act.reshape(slots, width)
    )
    down_t = lax.dot_general(rows_grad, hidden_act, (((0,), (1,)), ((), ())), preferred_element_type=F32)
    grad_gate, grad_up = final_grads(z.reshape(1), act_turned, first, second)
    return (grad_gate[None], grad_up[None], down_t.astype(BF16).T[None])


def solution(mesh):
    torus = Mesh(mesh.devices.reshape(4, 4, 2, mesh.shape["gy"]), ("gx_0", "gx_1", "gx_2", "gy"))
    return jax.shard_map(
        on_device,
        mesh=torus,
        in_specs=(
            P(GX, "gy"),
            P(GX, "gy"),
            P(GX, None, "gy"),
            P(GX, None, "gy"),
            P(GX, None),
            P(GX, None),
            P(GX, None, "gy"),
        ),
        out_specs=(P(GX, "gy", None), P(GX, "gy", None), P(GX, None, "gy")),
        check_vma=False,
    )
```

```python
import jax
import jax.numpy as jnp
from jax import lax
from jax.experimental import pallas as pl
from jax.experimental.pallas import tpu as pltpu
from jax.sharding import Mesh
from jax.sharding import PartitionSpec as P

MOST = 48
GX = ("gx_0", "gx_1", "gx_2")
F32 = jnp.float32
BF16 = jnp.bfloat16


def nt_dot(left, right):
    return lax.dot_general(left, right, (((1,), (1,)), ((), ())), preferred_element_type=F32)


def vmem_call(kernel, out_shapes, flops, size, scratch=(), limit=16 * 2**20):
    return pl.pallas_call(
        kernel,
        out_shape=out_shapes,
        scratch_shapes=scratch,
        cost_estimate=pl.CostEstimate(flops=flops, bytes_accessed=size, transcendentals=0),
        compiler_params=pltpu.CompilerParams(vmem_limit_bytes=limit),
    )


def placing(key_ref, e):
    rank = lax.broadcasted_iota(jnp.int32, (MOST, key_ref.shape[1]), 0)
    return key_ref[pl.ds(e, 1), :] == rank


def picking(place, ids_ref, e):
    chosen = [
        place * jnp.where(ids_ref[pl.ds(k, 1), :] == e, 1.0, 0.0) for k in range(ids_ref.shape[0])
    ]
    return jnp.concatenate(chosen, axis=1)


def pack_kernel(
    ids_hbm, weight_hbm, gate_hbm, up_hbm, grad_hbm, act_out, rows_out, key_ref,
    ids_ref, weight_ref, gate_ref, up_ref, grad_ref, both_ref, share_ref, sems,
):
    pairs = (
        (ids_hbm, ids_ref),
        (weight_hbm, weight_ref),
        (gate_hbm, gate_ref),
        (up_hbm, up_ref),
        (grad_hbm, grad_ref),
    )
    copies = [pltpu.make_async_copy(src, dst, sems.at[i]) for i, (src, dst) in enumerate(pairs)]
    for copy in copies:
        copy.start()
    copies[0].wait()
    copies[1].wait()
    experts, tokens = key_ref.shape
    tops = ids_ref.shape[0]
    half = gate_ref.shape[1]
    expert_at = lax.broadcasted_iota(jnp.int32, (experts, tokens), 0)
    named = jnp.zeros((experts, tokens), F32)
    share = jnp.zeros((experts, tokens), F32)
    for k in range(tops):
        hit = ids_ref[pl.ds(k, 1), :] == expert_at
        named = named + jnp.where(hit, 1.0, 0.0)
        share = share + jnp.where(hit, weight_ref[pl.ds(k, 1), :], 0.0)
    before = (
        lax.broadcasted_iota(jnp.int32, (tokens, tokens), 0)
        < lax.broadcasted_iota(jnp.int32, (tokens, tokens), 1)
    ).astype(F32)
    earlier = jnp.dot(named.astype(BF16), before.astype(BF16), preferred_element_type=F32)
    key_ref[...] = jnp.where(named > 0.5, earlier.astype(jnp.int32), -1)
    share_ref[...] = share
    copies[2].wait()
    copies[3].wait()
    for k in range(tops):
        at = slice(tokens * k, tokens * (k + 1))
        both_ref[:half, at] = gate_ref[k]
        both_ref[half:, at] = up_ref[k]
        gate = gate_ref[k].astype(F32)
        sig = 1.0 / (1.0 + jnp.exp(-gate))
        act_out[:, at] = (gate * sig * up_ref[k].astype(F32)).astype(BF16)
    copies[4].wait()
    group = 4

    def step(at, carry):
        places, scales, chosen = [], [], []
        for i in range(group):
            e = at * group + i
            mine = placing(key_ref, e)
            places.append(jnp.where(mine, 1.0, 0.0))
            scales.append(jnp.sum(jnp.where(mine, share_ref[pl.ds(e, 1), :], 0.0), axis=1, keepdims=True))
            chosen.append(picking(places[-1], ids_ref, e))
        place = jnp.concatenate(places, axis=0).astype(BF16)
        scale = jnp.concatenate(scales, axis=0)
        pick = jnp.concatenate(chosen, axis=0).astype(BF16)
        rows = pl.ds(pl.multiple_of(at * (group * MOST), group * MOST), group * MOST)
        rows_out[rows, : 2 * half] = nt_dot(pick, both_ref[...]).astype(BF16)
        rows_out[rows, 2 * half :] = (nt_dot(place, grad_ref[...]) * scale).astype(BF16)
        return carry

    lax.fori_loop(0, experts // group, step, 0)


def place_kernel(key_ref, values_ref, after_ref, out_ref):
    group = 4

    def step(at, carry):
        places = [jnp.where(placing(key_ref, at * group + i), 1.0, 0.0) for i in range(group)]
        rows = pl.ds(pl.multiple_of(at * (group * MOST), group * MOST), group * MOST)
        place = jnp.concatenate(places, axis=0).astype(BF16)
        out_ref[rows, :] = nt_dot(place, values_ref[...]).astype(BF16)
        return carry

    lax.fori_loop(0, key_ref.shape[0] // group, step, 0)


def spread_kernel(key_ref, ids_ref, values_ref, after_ref, out_ref):
    group = 4

    def step(at, carry):
        picks = []
        for i in range(group):
            e = at * group + i
            picks.append(picking(jnp.where(placing(key_ref, e), 1.0, 0.0), ids_ref, e))
        rows = pl.ds(pl.multiple_of(at * (group * MOST), group * MOST), group * MOST)
        pick = jnp.concatenate(picks, axis=0).astype(BF16)
        out_ref[rows, :] = nt_dot(pick, values_ref[...]).astype(BF16)
        return carry

    lax.fori_loop(0, key_ref.shape[0] // group, step, 0)


def turn_kernel(rows_ref, out_ref):
    out_ref[...] = rows_ref[...].astype(F32).T.astype(BF16)


def weight_kernel(at_ref, weight_ref, out_ref, turned_ref):
    turned_ref[...] = weight_ref[...].astype(F32).T.astype(BF16)
    z = at_ref[0]
    planes = 16
    share = out_ref.shape[0] // planes
    for j in range(planes):
        start = pl.multiple_of(lax.rem(z + j, planes) * share, share)
        out_ref[j * share : (j + 1) * share, :] = turned_ref[pl.ds(start, share), :]


def sums_kernel(rows_ref, weight_ref, grad_ref, upper_ref, gated_ref, *chunk_refs):
    half = upper_ref.shape[0]
    grad_ref[...] = rows_ref[:, 2 * half :]
    group = 4
    for at in range(0, len(chunk_refs), group):
        sums = nt_dot(weight_ref[at * half : (at + group) * half, :], grad_ref[...]).astype(BF16)
        for i in range(group):
            chunk_refs[at + i][...] = sums[half * i : half * (i + 1), :]
    both = rows_ref[:, : 2 * half].astype(F32).T
    gate = both[:half]
    up = both[half:]
    sig = 1.0 / (1.0 + jnp.exp(-gate))
    upper_ref[...] = gate * sig
    gated_ref[...] = up * sig * (1.0 + gate * (1.0 - sig))


def late_kernel(moving_ref, own_ref, after_ref, out_ref):
    out_ref[...] = (moving_ref[...].astype(F32) + own_ref[...].astype(F32)).astype(BF16)


def scale_kernel(ahead_ref, behind_ref, own_ref, upper_ref, gated_ref, out_ref):
    half = ahead_ref.shape[0]
    total = ahead_ref[...].astype(F32) + behind_ref[...].astype(F32) + own_ref[...].astype(F32)
    out_ref[:half, :] = (total * gated_ref[...]).astype(BF16)
    out_ref[half:, :] = (total * upper_ref[...]).astype(BF16)


def final_kernel(act_ref, both_ref, gate_out, up_out):
    count, both, slots = both_ref.shape
    half = both // 2
    gate_out[...] = nt_dot(act_ref[...], both_ref[:, :half, :].reshape(count * half, slots)).astype(BF16)
    up_out[...] = nt_dot(act_ref[...], both_ref[:, half:, :].reshape(count * half, slots)).astype(BF16)


def final_grads(act_turned, gathered):
    width, slots = act_turned.shape
    planes, both, _ = gathered.shape
    group = 4
    spec = pl.BlockSpec((width, group * both // 2), lambda i: (0, i))
    shape = jax.ShapeDtypeStruct((width, planes * both // 2), BF16)
    return pl.pallas_call(
        final_kernel,
        grid=(planes // group,),
        in_specs=[
            pl.BlockSpec((width, slots), lambda i: (0, 0)),
            pl.BlockSpec((group, both, slots), lambda i: (i, 0, 0)),
        ],
        out_specs=[spec, spec],
        out_shape=[shape, shape],
        cost_estimate=pl.CostEstimate(
            flops=2 * width * slots * planes * both, bytes_accessed=2 * slots * planes * both, transcendentals=0
        ),
        compiler_params=pltpu.CompilerParams(vmem_limit_bytes=60 * 2**20),
    )(act_turned, gathered)


def add(moving, own):
    return (moving.astype(F32) + own.astype(F32)).astype(BF16)


def ring_pairs(count):
    return (
        [(i, (i + 1) % count) for i in range(count)],
        [(i, (i - 1) % count) for i in range(count)],
    )


def add_after(moving, own, after):
    return pl.pallas_call(
        late_kernel,
        in_specs=[pl.BlockSpec(memory_space=pltpu.VMEM)] * 2 + [pl.BlockSpec(memory_space=pl.ANY)],
        out_shape=jax.ShapeDtypeStruct(moving.shape, moving.dtype),
        cost_estimate=pl.CostEstimate(flops=moving.size, bytes_accessed=6 * moving.size, transcendentals=0),
        compiler_params=pltpu.CompilerParams(vmem_limit_bytes=4 * 2**20),
    )(moving, own, after)


def ring_sums(chunks, axis, early, late, beside):
    count = len(chunks)
    far = count // 2
    plus, minus = ring_pairs(count)
    ahead, behind = (chunks[far], chunks[far + 1])
    for s in range(far):
        ahead = lax.ppermute(ahead, axis, plus)
        if s < far - 1:
            behind = lax.ppermute(behind, axis, minus)
            if s == late:
                ahead = add_after(ahead, chunks[far - 1 - s], other)
            else:
                ahead = add(ahead, chunks[far - 1 - s])
        if s < far - 2:
            behind = add(behind, chunks[far + 2 + s])
        if s == early:
            other = beside(behind)
    return ahead, behind, other


def on_device(activations, out_grad, saved_gate, saved_up, route_ids, route_weight, down_weight):
    experts = lax.axis_size(GX)
    planes = lax.axis_size("gy")
    z = lax.axis_index("gy")
    tokens, width = activations.shape
    tops = route_ids.shape[1]
    slots = experts * MOST
    half = saved_gate.shape[2]
    hidden = down_weight.shape[1]
    sds = jax.ShapeDtypeStruct
    ids = route_ids.T
    gate = jnp.transpose(saved_gate, (1, 2, 0))
    up = jnp.transpose(saved_up, (1, 2, 0))
    hbm = pl.BlockSpec(memory_space=pltpu.MemorySpace.HBM)
    act_share, routes, key = pl.pallas_call(
        pack_kernel,
        in_specs=[hbm] * 5,
        out_shape=[
            sds((half, tops * tokens), BF16),
            sds((slots, 2 * half + width), BF16),
            sds((experts, tokens), jnp.int32),
        ],
        scratch_shapes=[
            pltpu.VMEM((tops, tokens), jnp.int32),
            pltpu.VMEM((tops, tokens), F32),
            pltpu.VMEM((tops, half, tokens), BF16),
            pltpu.VMEM((tops, half, tokens), BF16),
            pltpu.VMEM((width, tokens), BF16),
            pltpu.VMEM((2 * half, tops * tokens), BF16),
            pltpu.VMEM((experts, tokens), F32),
            pltpu.SemaphoreType.DMA((5,)),
        ],
        cost_estimate=pl.CostEstimate(
            flops=2 * slots * tokens * (width + 16 * half), bytes_accessed=4 * slots * width, transcendentals=0
        ),
        compiler_params=pltpu.CompilerParams(vmem_limit_bytes=60 * 2**20),
    )(ids, route_weight.T, gate, up, out_grad.T)
    hidden_act = lax.all_gather(act_share, "gy", axis=0, tiled=True)
    turned = pl.pallas_call(
        weight_kernel,
        in_specs=[pl.BlockSpec(memory_space=pltpu.SMEM), pl.BlockSpec(memory_space=pltpu.VMEM)],
        out_shape=sds((hidden, width), BF16),
        scratch_shapes=[pltpu.VMEM((hidden, width), BF16)],
        cost_estimate=pl.CostEstimate(flops=0, bytes_accessed=6 * hidden * width, transcendentals=0),
        compiler_params=pltpu.CompilerParams(vmem_limit_bytes=16 * 2**20),
    )(z.reshape(1), down_weight[0].T)
    rows = lax.all_to_all(routes.reshape(experts, MOST, -1), GX, 0, 0, tiled=True).reshape(slots, -1)
    rows_grad, upper_by, gated_by, *chunks = vmem_call(
        sums_kernel,
        [sds((slots, width), BF16), sds((half, slots), F32), sds((half, slots), F32)]
        + [sds((half, slots), BF16)] * planes,
        2 * hidden * slots * width,
        8 * slots * width,
        limit=60 * 2**20,
    )(rows, turned)

    def beside(mark):
        act_routes = vmem_call(
            place_kernel, sds((slots, width), BF16), 2 * slots * tokens * width, 2 * slots * width
        )(key, activations.T, mark)
        return lax.all_to_all(act_routes.reshape(experts, MOST, -1), GX, 0, 0, tiled=True)

    ahead, behind, rows_act = ring_sums(chunks, "gy", 1, 5, beside)
    both = vmem_call(
        scale_kernel, sds((2 * half, slots), BF16), 4 * half * slots, 20 * half * slots
    )(ahead, behind, chunks[0], upper_by, gated_by)
    gathered = lax.all_gather(both, "gy", axis=0)
    act_turned = vmem_call(turn_kernel, sds((width, slots), BF16), 0, 4 * slots * width)(
        rows_act.reshape(slots, width)
    )
    spread = vmem_call(
        spread_kernel, sds((slots, hidden), BF16), 2 * slots * hidden * tops * tokens, 4 * slots * hidden
    )(key, ids, hidden_act, both)
    rows_hidden = lax.all_to_all(spread.reshape(experts, MOST, -1), GX, 0, 0, tiled=True)
    down_t = lax.dot_general(
        rows_grad, rows_hidden.reshape(slots, hidden), (((0,), (0,)), ((), ())), preferred_element_type=F32
    )
    grad_gate, grad_up = final_grads(act_turned, gathered)
    return (grad_gate[None], grad_up[None], down_t.astype(BF16).T[None])


def solution(mesh):
    torus = Mesh(mesh.devices.reshape(4, 4, 2, mesh.shape["gy"]), ("gx_0", "gx_1", "gx_2", "gy"))
    return jax.shard_map(
        on_device,
        mesh=torus,
        in_specs=(
            P(GX, "gy"),
            P(GX, "gy"),
            P(GX, None, "gy"),
            P(GX, None, "gy"),
            P(GX, None),
            P(GX, None),
            P(GX, None, "gy"),
        ),
        out_specs=(P(GX, "gy", None), P(GX, "gy", None), P(GX, None, "gy")),
        check_vma=False,
    )
```

```python
import jax
import jax.numpy as jnp
from jax import lax
from jax.experimental import pallas as pl
from jax.experimental.pallas import tpu as pltpu
from jax.sharding import Mesh
from jax.sharding import PartitionSpec as P

MOST = 48
GX = ("gx_0", "gx_1", "gx_2")
F32 = jnp.float32
BF16 = jnp.bfloat16


def nt_dot(left, right):
    return lax.dot_general(left, right, (((1,), (1,)), ((), ())), preferred_element_type=F32)


def vmem_call(kernel, out_shapes, flops, size, scratch=(), limit=16 * 2**20):
    return pl.pallas_call(
        kernel,
        out_shape=out_shapes,
        scratch_shapes=scratch,
        cost_estimate=pl.CostEstimate(flops=flops, bytes_accessed=size, transcendentals=0),
        compiler_params=pltpu.CompilerParams(vmem_limit_bytes=limit),
    )


def placing(key_ref, e):
    rank = lax.broadcasted_iota(jnp.int32, (MOST, key_ref.shape[1]), 0)
    return key_ref[pl.ds(e, 1), :] == rank


def picking(place, ids_ref, e):
    chosen = [
        place * jnp.where(ids_ref[pl.ds(k, 1), :] == e, 1.0, 0.0) for k in range(ids_ref.shape[0])
    ]
    return jnp.concatenate(chosen, axis=1)


def pack_kernel(
    ids_hbm, weight_hbm, gate_hbm, up_hbm, grad_hbm, act_out, rows_out, key_ref, both_ref,
    ids_ref, weight_ref, gate_ref, up_ref, grad_ref, share_ref, sems,
):
    pairs = (
        (ids_hbm, ids_ref),
        (weight_hbm, weight_ref),
        (gate_hbm, gate_ref),
        (up_hbm, up_ref),
        (grad_hbm, grad_ref),
    )
    copies = [pltpu.make_async_copy(src, dst, sems.at[i]) for i, (src, dst) in enumerate(pairs)]
    for copy in copies:
        copy.start()
    copies[0].wait()
    copies[1].wait()
    experts, tokens = key_ref.shape
    tops = ids_ref.shape[0]
    half = gate_ref.shape[1]
    expert_at = lax.broadcasted_iota(jnp.int32, (experts, tokens), 0)
    named = jnp.zeros((experts, tokens), F32)
    share = jnp.zeros((experts, tokens), F32)
    for k in range(tops):
        hit = ids_ref[pl.ds(k, 1), :] == expert_at
        named = named + jnp.where(hit, 1.0, 0.0)
        share = share + jnp.where(hit, weight_ref[pl.ds(k, 1), :], 0.0)
    before = (
        lax.broadcasted_iota(jnp.int32, (tokens, tokens), 0)
        < lax.broadcasted_iota(jnp.int32, (tokens, tokens), 1)
    ).astype(F32)
    earlier = jnp.dot(named.astype(BF16), before.astype(BF16), preferred_element_type=F32)
    key_ref[...] = jnp.where(named > 0.5, earlier.astype(jnp.int32), -1)
    share_ref[...] = share
    copies[2].wait()
    copies[3].wait()
    for k in range(tops):
        at = slice(tokens * k, tokens * (k + 1))
        both_ref[:half, at] = gate_ref[k]
        both_ref[half:, at] = up_ref[k]
        gate = gate_ref[k].astype(F32)
        sig = 1.0 / (1.0 + jnp.exp(-gate))
        act_out[:, at] = (gate * sig * up_ref[k].astype(F32)).astype(BF16)
    copies[4].wait()
    group = 4

    def step(at, carry):
        places, scales = [], []
        for i in range(group):
            e = at * group + i
            mine = placing(key_ref, e)
            places.append(jnp.where(mine, 1.0, 0.0))
            scales.append(jnp.sum(jnp.where(mine, share_ref[pl.ds(e, 1), :], 0.0), axis=1, keepdims=True))
        place = jnp.concatenate(places, axis=0).astype(BF16)
        scale = jnp.concatenate(scales, axis=0)
        rows = pl.ds(pl.multiple_of(at * (group * MOST), group * MOST), group * MOST)
        rows_out[rows, :] = (nt_dot(place, grad_ref[...]) * scale).astype(BF16)
        return carry

    lax.fori_loop(0, experts // group, step, 0)


def place_kernel(key_ref, ids_ref, both_ref, values_ref, after_ref, out_ref):
    group = 4
    both = both_ref.shape[0]

    def step(at, carry):
        places, picks = [], []
        for i in range(group):
            e = at * group + i
            places.append(jnp.where(placing(key_ref, e), 1.0, 0.0))
            picks.append(picking(places[-1], ids_ref, e))
        rows = pl.ds(pl.multiple_of(at * (group * MOST), group * MOST), group * MOST)
        place = jnp.concatenate(places, axis=0).astype(BF16)
        pick = jnp.concatenate(picks, axis=0).astype(BF16)
        out_ref[rows, :both] = nt_dot(pick, both_ref[...]).astype(BF16)
        out_ref[rows, both:] = nt_dot(place, values_ref[...]).astype(BF16)
        return carry

    lax.fori_loop(0, key_ref.shape[0] // group, step, 0)


def spread_kernel(key_ref, ids_ref, values_ref, after_ref, out_ref):
    group = 4

    def step(at, carry):
        picks = []
        for i in range(group):
            e = at * group + i
            picks.append(picking(jnp.where(placing(key_ref, e), 1.0, 0.0), ids_ref, e))
        rows = pl.ds(pl.multiple_of(at * (group * MOST), group * MOST), group * MOST)
        pick = jnp.concatenate(picks, axis=0).astype(BF16)
        out_ref[rows, :] = nt_dot(pick, values_ref[...]).astype(BF16)
        return carry

    lax.fori_loop(0, key_ref.shape[0] // group, step, 0)


def weight_kernel(at_ref, weight_ref, out_ref, turned_ref):
    turned_ref[...] = weight_ref[...].astype(F32).T.astype(BF16)
    planes = 16
    share = out_ref.shape[0] // planes
    for j in range(planes):
        chunk = lax.rem(at_ref[0] + at_ref[1] * j, planes)
        out_ref[j * share : (j + 1) * share, :] = turned_ref[
            pl.ds(pl.multiple_of(chunk * share, share), share), :
        ]


def sums_kernel(grad_ref, weight_ref, *chunk_refs):
    half = chunk_refs[0].shape[0]
    group = 4
    for at in range(0, len(chunk_refs), group):
        sums = nt_dot(weight_ref[at * half : (at + group) * half, :], grad_ref[...]).astype(BF16)
        for i in range(group):
            chunk_refs[at + i][...] = sums[half * i : half * (i + 1), :]


def unpack_kernel(rows_ref, act_ref, upper_ref, gated_ref):
    half = upper_ref.shape[0]
    act_ref[...] = rows_ref[:, 2 * half :].astype(F32).T.astype(BF16)
    both = rows_ref[:, : 2 * half].astype(F32).T
    gate = both[:half]
    up = both[half:]
    sig = 1.0 / (1.0 + jnp.exp(-gate))
    upper_ref[...] = gate * sig
    gated_ref[...] = up * sig * (1.0 + gate * (1.0 - sig))


def late_kernel(moving_ref, own_ref, after_ref, out_ref):
    out_ref[...] = (moving_ref[...].astype(F32) + own_ref[...].astype(F32)).astype(BF16)


def scale_kernel(ahead_ref, behind_ref, own_ref, upper_ref, gated_ref, out_ref):
    half = ahead_ref.shape[0]
    total = ahead_ref[...].astype(F32) + behind_ref[...].astype(F32) + own_ref[...].astype(F32)
    out_ref[:half, :] = (total * gated_ref[...]).astype(BF16)
    out_ref[half:, :] = (total * upper_ref[...]).astype(BF16)


def final_kernel(act_ref, both_ref, gate_out, up_out):
    count, both, slots = both_ref.shape
    half = both // 2
    gate_out[...] = nt_dot(act_ref[...], both_ref[:, :half, :].reshape(count * half, slots)).astype(BF16)
    up_out[...] = nt_dot(act_ref[...], both_ref[:, half:, :].reshape(count * half, slots)).astype(BF16)


def final_grads(act_turned, gathered):
    width, slots = act_turned.shape
    planes, both, _ = gathered.shape
    group = 4
    spec = pl.BlockSpec((width, group * both // 2), lambda i: (0, i))
    shape = jax.ShapeDtypeStruct((width, planes * both // 2), BF16)
    return pl.pallas_call(
        final_kernel,
        grid=(planes // group,),
        in_specs=[
            pl.BlockSpec((width, slots), lambda i: (0, 0)),
            pl.BlockSpec((group, both, slots), lambda i: (i, 0, 0)),
        ],
        out_specs=[spec, spec],
        out_shape=[shape, shape],
        cost_estimate=pl.CostEstimate(
            flops=2 * width * slots * planes * both, bytes_accessed=2 * slots * planes * both, transcendentals=0
        ),
        compiler_params=pltpu.CompilerParams(vmem_limit_bytes=60 * 2**20),
    )(act_turned, gathered)


def add(moving, own):
    return (moving.astype(F32) + own.astype(F32)).astype(BF16)


def ring_pairs(count, step):
    pairs = [(i, (i + step) % count) for i in range(count)]
    return pairs + [(count + (i + step) % count, count + i) for i in range(count)]


def add_after(moving, own, after):
    return pl.pallas_call(
        late_kernel,
        in_specs=[pl.BlockSpec(memory_space=pltpu.VMEM)] * 2 + [pl.BlockSpec(memory_space=pl.ANY)],
        out_shape=jax.ShapeDtypeStruct(moving.shape, moving.dtype),
        cost_estimate=pl.CostEstimate(flops=moving.size, bytes_accessed=6 * moving.size, transcendentals=0),
        compiler_params=pltpu.CompilerParams(vmem_limit_bytes=4 * 2**20),
    )(moving, own, after)


def ring_sums(chunks, axis, early, late, beside):
    count = len(chunks)
    far = count // 2
    plus, minus = (ring_pairs(count, 1), ring_pairs(count, -1))
    ahead, behind = (chunks[far], chunks[far + 1])
    for s in range(far):
        ahead = lax.ppermute(ahead, axis, plus)
        if s < far - 1:
            behind = lax.ppermute(behind, axis, minus)
            if s == late:
                ahead = add_after(ahead, chunks[far - 1 - s], other)
            else:
                ahead = add(ahead, chunks[far - 1 - s])
        if s < far - 2:
            behind = add(behind, chunks[far + 2 + s])
        if s == early:
            other = beside(behind)
    return ahead, behind, other


def on_device(activations, out_grad, saved_gate, saved_up, route_ids, route_weight, down_weight):
    experts = lax.axis_size(GX)
    planes = lax.axis_size("gy")
    z = lax.axis_index("gy")
    tokens, width = activations.shape
    tops = route_ids.shape[1]
    slots = experts * MOST
    half = saved_gate.shape[2]
    hidden = down_weight.shape[1]
    sds = jax.ShapeDtypeStruct
    ids = route_ids.T
    gate = jnp.transpose(saved_gate, (1, 2, 0))
    up = jnp.transpose(saved_up, (1, 2, 0))
    hbm = pl.BlockSpec(memory_space=pltpu.MemorySpace.HBM)
    act_share, routes, key, gate_up = pl.pallas_call(
        pack_kernel,
        in_specs=[hbm] * 5,
        out_shape=[
            sds((half, tops * tokens), BF16),
            sds((slots, width), BF16),
            sds((experts, tokens), jnp.int32),
            sds((2 * half, tops * tokens), BF16),
        ],
        scratch_shapes=[
            pltpu.VMEM((tops, tokens), jnp.int32),
            pltpu.VMEM((tops, tokens), F32),
            pltpu.VMEM((tops, half, tokens), BF16),
            pltpu.VMEM((tops, half, tokens), BF16),
            pltpu.VMEM((width, tokens), BF16),
            pltpu.VMEM((experts, tokens), F32),
            pltpu.SemaphoreType.DMA((5,)),
        ],
        cost_estimate=pl.CostEstimate(
            flops=2 * slots * tokens * (width + 16 * half), bytes_accessed=4 * slots * width, transcendentals=0
        ),
        compiler_params=pltpu.CompilerParams(vmem_limit_bytes=60 * 2**20),
    )(ids, route_weight.T, gate, up, out_grad.T)
    hidden_act = lax.all_gather(act_share, "gy", axis=0, tiled=True)
    turned = pl.pallas_call(
        weight_kernel,
        in_specs=[pl.BlockSpec(memory_space=pltpu.SMEM), pl.BlockSpec(memory_space=pltpu.VMEM)],
        out_shape=sds((hidden, width), BF16),
        scratch_shapes=[pltpu.VMEM((hidden, width), BF16)],
        cost_estimate=pl.CostEstimate(flops=0, bytes_accessed=6 * hidden * width, transcendentals=0),
        compiler_params=pltpu.CompilerParams(vmem_limit_bytes=16 * 2**20),
    )(jnp.stack([z, 1 + (planes - 2) * lax.axis_index(GX[-1])]), down_weight[0].T)
    rows_grad = lax.all_to_all(routes.reshape(experts, MOST, -1), GX, 0, 0, tiled=True).reshape(slots, -1)
    chunks = vmem_call(
        sums_kernel,
        [sds((half, slots), BF16)] * planes,
        2 * hidden * slots * width,
        6 * slots * width,
        limit=60 * 2**20,
    )(rows_grad, turned)

    def beside(mark):
        packed = vmem_call(
            place_kernel,
            sds((slots, 2 * half + width), BF16),
            2 * slots * tokens * (width + 16 * half),
            2 * slots * width,
        )(key, ids, gate_up, activations.T, mark)
        return lax.all_to_all(packed.reshape(experts, MOST, -1), GX, 0, 0, tiled=True)

    ahead, behind, rows_act = ring_sums(chunks, ("gx_2", "gy"), 1, 5, beside)
    act_turned, upper_by, gated_by = vmem_call(
        unpack_kernel,
        [sds((width, slots), BF16), sds((half, slots), F32), sds((half, slots), F32)],
        20 * half * slots,
        6 * slots * width,
    )(rows_act.reshape(slots, -1))
    both = vmem_call(
        scale_kernel, sds((2 * half, slots), BF16), 4 * half * slots, 20 * half * slots
    )(ahead, behind, chunks[0], upper_by, gated_by)
    gathered = lax.all_gather(both, "gy", axis=0)
    spread = vmem_call(
        spread_kernel, sds((slots, hidden), BF16), 2 * slots * hidden * tops * tokens, 4 * slots * hidden
    )(key, ids, hidden_act, both)
    rows_hidden = lax.all_to_all(spread.reshape(experts, MOST, -1), GX, 0, 0, tiled=True)
    down_t = lax.dot_general(
        rows_grad, rows_hidden.reshape(slots, hidden), (((0,), (0,)), ((), ())), preferred_element_type=F32
    )
    grad_gate, grad_up = final_grads(act_turned, gathered)
    return (grad_gate[None], grad_up[None], down_t.astype(BF16).T[None])


def solution(mesh):
    torus = Mesh(mesh.devices.reshape(4, 4, 2, mesh.shape["gy"]), ("gx_0", "gx_1", "gx_2", "gy"))
    return jax.shard_map(
        on_device,
        mesh=torus,
        in_specs=(
            P(GX, "gy"),
            P(GX, "gy"),
            P(GX, None, "gy"),
            P(GX, None, "gy"),
            P(GX, None),
            P(GX, None),
            P(GX, None, "gy"),
        ),
        out_specs=(P(GX, "gy", None), P(GX, "gy", None), P(GX, None, "gy")),
        check_vma=False,
    )
```

```python
import jax
import jax.numpy as jnp
from jax import lax
from jax.experimental import pallas as pl
from jax.experimental.pallas import tpu as pltpu
from jax.sharding import Mesh
from jax.sharding import PartitionSpec as P

MOST = 48
GX = ("gx_0", "gx_1", "gx_2")
F32 = jnp.float32
BF16 = jnp.bfloat16


def nt_dot(left, right):
    return lax.dot_general(left, right, (((1,), (1,)), ((), ())), preferred_element_type=F32)


def placing(key_ref, e):
    rank = lax.broadcasted_iota(jnp.int32, (MOST, key_ref.shape[1]), 0)
    return key_ref[pl.ds(e, 1), :] == rank


def picking(place, ids_ref, e):
    chosen = [
        place * jnp.where(ids_ref[pl.ds(k, 1), :] == e, 1.0, 0.0) for k in range(ids_ref.shape[0])
    ]
    return jnp.concatenate(chosen, axis=1)


def pack_kernel(
    ids_hbm, weight_hbm, gate_hbm, up_hbm, grad_hbm, act_out, rows_out, key_ref, both_ref,
    ids_ref, weight_ref, gate_ref, up_ref, grad_ref, share_ref, sems,
):
    pairs = (
        (ids_hbm, ids_ref),
        (weight_hbm, weight_ref),
        (gate_hbm, gate_ref),
        (up_hbm, up_ref),
        (grad_hbm, grad_ref),
    )
    copies = [pltpu.make_async_copy(src, dst, sems.at[i]) for i, (src, dst) in enumerate(pairs)]
    for copy in copies:
        copy.start()
    copies[0].wait()
    copies[1].wait()
    experts, tokens = key_ref.shape
    tops = ids_ref.shape[0]
    half = gate_ref.shape[1]
    expert_at = lax.broadcasted_iota(jnp.int32, (experts, tokens), 0)
    named = jnp.zeros((experts, tokens), F32)
    share = jnp.zeros((experts, tokens), F32)
    for k in range(tops):
        hit = ids_ref[pl.ds(k, 1), :] == expert_at
        named = named + jnp.where(hit, 1.0, 0.0)
        share = share + jnp.where(hit, weight_ref[pl.ds(k, 1), :], 0.0)
    before = (
        lax.broadcasted_iota(jnp.int32, (tokens, tokens), 0)
        < lax.broadcasted_iota(jnp.int32, (tokens, tokens), 1)
    ).astype(F32)
    earlier = jnp.dot(named.astype(BF16), before.astype(BF16), preferred_element_type=F32)
    key_ref[...] = jnp.where(named > 0.5, earlier.astype(jnp.int32), -1)
    share_ref[...] = share
    copies[2].wait()
    copies[3].wait()
    for k in range(tops):
        at = slice(tokens * k, tokens * (k + 1))
        both_ref[:half, at] = gate_ref[k]
        both_ref[half:, at] = up_ref[k]
        gate = gate_ref[k].astype(F32)
        sig = 1.0 / (1.0 + jnp.exp(-gate))
        act_out[:, at] = (gate * sig * up_ref[k].astype(F32)).astype(BF16)
    copies[4].wait()
    group = 4

    def step(at, carry):
        places, scales = [], []
        for i in range(group):
            e = at * group + i
            mine = placing(key_ref, e)
            places.append(jnp.where(mine, 1.0, 0.0))
            scales.append(jnp.sum(jnp.where(mine, share_ref[pl.ds(e, 1), :], 0.0), axis=1, keepdims=True))
        place = jnp.concatenate(places, axis=0).astype(BF16)
        scale = jnp.concatenate(scales, axis=0)
        rows = pl.ds(pl.multiple_of(at * (group * MOST), group * MOST), group * MOST)
        rows_out[rows, :] = (nt_dot(place, grad_ref[...]) * scale).astype(BF16)
        return carry

    lax.fori_loop(0, experts // group, step, 0)


def place_kernel(key_ref, ids_ref, both_ref, values_ref, sums_ref, out_ref):
    group = 4
    both = both_ref.shape[0]

    def step(at, carry):
        places, picks = [], []
        for i in range(group):
            e = at * group + i
            places.append(jnp.where(placing(key_ref, e), 1.0, 0.0))
            picks.append(picking(places[-1], ids_ref, e))
        rows = pl.ds(pl.multiple_of(at * (group * MOST), group * MOST), group * MOST)
        place = jnp.concatenate(places, axis=0).astype(BF16)
        pick = jnp.concatenate(picks, axis=0).astype(BF16)
        out_ref[rows, :both] = nt_dot(pick, both_ref[...]).astype(BF16)
        out_ref[rows, both:] = nt_dot(place, values_ref[...]).astype(BF16)
        return carry

    lax.fori_loop(0, key_ref.shape[0] // group, step, 0)


def spread_kernel(at_ref, key_ref, ids_ref, after_ref, *refs):
    pieces, out_ref, values_ref = refs[:-2], refs[-2], refs[-1]
    group = 4
    share = pieces[0].shape[0]
    for r, piece in enumerate(pieces):
        plane = lax.rem(at_ref[0] + r, len(pieces))
        values_ref[pl.ds(pl.multiple_of(plane * share, share), share), :] = piece[...]

    def step(at, carry):
        picks = []
        for i in range(group):
            e = at * group + i
            picks.append(picking(jnp.where(placing(key_ref, e), 1.0, 0.0), ids_ref, e))
        rows = pl.ds(pl.multiple_of(at * (group * MOST), group * MOST), group * MOST)
        pick = jnp.concatenate(picks, axis=0).astype(BF16)
        out_ref[rows, :] = nt_dot(pick, values_ref[...]).astype(BF16)
        return carry

    lax.fori_loop(0, key_ref.shape[0] // group, step, 0)


def weight_kernel(weight_ref, ahead_ref, behind_ref, out_ref):
    out_ref[...] = weight_ref[...].astype(F32).T.astype(BF16)


def unpack_kernel(rows_ref, ahead_ref, behind_ref, act_ref, upper_ref, gated_ref):
    half = upper_ref.shape[0]
    act_ref[...] = rows_ref[:, 2 * half :].astype(F32).T.astype(BF16)
    both = rows_ref[:, : 2 * half].astype(F32).T
    gate = both[:half]
    up = both[half:]
    sig = 1.0 / (1.0 + jnp.exp(-gate))
    upper_ref[...] = gate * sig
    gated_ref[...] = up * sig * (1.0 + gate * (1.0 - sig))


def scale_kernel(total_ref, upper_ref, gated_ref, after_ref, out_ref):
    half = total_ref.shape[0]
    total = total_ref[...].astype(F32)
    out_ref[:half, :] = (total * gated_ref[...]).astype(BF16)
    out_ref[half:, :] = (total * upper_ref[...]).astype(BF16)


def final_kernel(act_ref, both_ref, gate_out, up_out):
    count, both, slots = both_ref.shape
    half = both // 2
    gate_out[...] = nt_dot(act_ref[...], both_ref[:, :half, :].reshape(count * half, slots)).astype(BF16)
    up_out[...] = nt_dot(act_ref[...], both_ref[:, half:, :].reshape(count * half, slots)).astype(BF16)


def final_grads(act_turned, gathered):
    width, slots = act_turned.shape
    planes, both, _ = gathered.shape
    group = 4
    spec = pl.BlockSpec((width, group * both // 2), lambda i: (0, i))
    shape = jax.ShapeDtypeStruct((width, planes * both // 2), BF16)
    return pl.pallas_call(
        final_kernel,
        grid=(planes // group,),
        in_specs=[
            pl.BlockSpec((width, slots), lambda i: (0, 0)),
            pl.BlockSpec((group, both, slots), lambda i: (i, 0, 0)),
        ],
        out_specs=[spec, spec],
        out_shape=[shape, shape],
        cost_estimate=pl.CostEstimate(
            flops=2 * width * slots * planes * both, bytes_accessed=2 * slots * planes * both, transcendentals=0
        ),
        compiler_params=pltpu.CompilerParams(vmem_limit_bytes=59 * 2**20),
    )(act_turned, gathered)


def hold_kernel(value_ref, after_ref, out_ref):
    out_ref[...] = value_ref[...]


def hold(value, after):
    return pl.pallas_call(
        hold_kernel,
        in_specs=[pl.BlockSpec(memory_space=pltpu.VMEM), pl.BlockSpec(memory_space=pl.ANY)],
        out_shape=jax.ShapeDtypeStruct(value.shape, value.dtype),
        cost_estimate=pl.CostEstimate(flops=0, bytes_accessed=4 * value.size, transcendentals=0),
        compiler_params=pltpu.CompilerParams(vmem_limit_bytes=4 * 2**20),
    )(value, after)


def ring_rounds(ahead, behind, axis, rounds, both_ways):
    count = lax.axis_size(axis)
    plus = [(i, (i + 1) % count) for i in range(count)]
    minus = [(i, (i - 1) % count) for i in range(count)]
    before, after = [], []
    for s in range(rounds):
        ahead = lax.ppermute(ahead, axis, plus)
        before.append(ahead)
        if s < both_ways:
            behind = lax.ppermute(behind, axis, minus)
            after.append(behind)
    return before, after


def on_device(activations, out_grad, saved_gate, saved_up, route_ids, route_weight, down_weight):
    experts = lax.axis_size(GX)
    planes = lax.axis_size("gy")
    z = lax.axis_index("gy")
    tokens, width = activations.shape
    tops = route_ids.shape[1]
    slots = experts * MOST
    half = saved_gate.shape[2]
    hidden = down_weight.shape[1]
    sds = jax.ShapeDtypeStruct
    ids = route_ids.T
    gate = jnp.transpose(saved_gate, (1, 2, 0))
    up = jnp.transpose(saved_up, (1, 2, 0))
    hbm = pl.BlockSpec(memory_space=pltpu.MemorySpace.HBM)
    act_share, routes, key, gate_up = pl.pallas_call(
        pack_kernel,
        in_specs=[hbm] * 5,
        out_shape=[
            sds((half, tops * tokens), BF16),
            sds((slots, width), BF16),
            sds((experts, tokens), jnp.int32),
            sds((2 * half, tops * tokens), BF16),
        ],
        scratch_shapes=[
            pltpu.VMEM((tops, tokens), jnp.int32),
            pltpu.VMEM((tops, tokens), F32),
            pltpu.VMEM((tops, half, tokens), BF16),
            pltpu.VMEM((tops, half, tokens), BF16),
            pltpu.VMEM((width, tokens), BF16),
            pltpu.VMEM((experts, tokens), F32),
            pltpu.SemaphoreType.DMA((5,)),
        ],
        cost_estimate=pl.CostEstimate(
            flops=2 * slots * tokens * (width + 16 * half), bytes_accessed=4 * slots * width, transcendentals=0
        ),
        compiler_params=pltpu.CompilerParams(vmem_limit_bytes=60 * 2**20),
    )(ids, route_weight.T, gate, up, out_grad.T)
    early = 2
    before, after = ring_rounds(act_share, act_share, "gy", early, early)
    turned = pl.pallas_call(
        weight_kernel,
        in_specs=[pl.BlockSpec(memory_space=pltpu.VMEM)] + [pl.BlockSpec(memory_space=pl.ANY)] * 2,
        out_shape=sds((hidden, width), BF16),
        cost_estimate=pl.CostEstimate(flops=0, bytes_accessed=6 * hidden * width, transcendentals=0),
        compiler_params=pltpu.CompilerParams(vmem_limit_bytes=16 * 2**20),
    )(down_weight[0].T, before[-1], after[-1])
    rows_grad = lax.all_to_all(routes.reshape(experts, MOST, -1), GX, 0, 0, tiled=True).reshape(slots, -1)
    sums = nt_dot(turned, rows_grad).astype(BF16)
    total = lax.psum_scatter(sums, "gy", scatter_dimension=0, tiled=True)
    packed = pl.pallas_call(
        place_kernel,
        in_specs=[pl.BlockSpec(memory_space=pltpu.VMEM)] * 4 + [pl.BlockSpec(memory_space=pl.ANY)],
        out_shape=sds((slots, 2 * half + width), BF16),
        cost_estimate=pl.CostEstimate(
            flops=2 * slots * tokens * (width + 16 * half), bytes_accessed=2 * slots * width, transcendentals=0
        ),
        compiler_params=pltpu.CompilerParams(vmem_limit_bytes=16 * 2**20),
    )(key, ids, gate_up, activations.T, sums)
    late = planes // 2 - early
    before_late, after_late = ring_rounds(hold(before[-1], packed), after[-1], "gy", late, late - 1)
    act_pieces = [act_share] + after + after_late + (before + before_late)[::-1]
    rows_act = lax.all_to_all(packed.reshape(experts, MOST, -1), GX, 0, 0, tiled=True)
    vmem = pl.BlockSpec(memory_space=pltpu.VMEM)
    anywhere = pl.BlockSpec(memory_space=pl.ANY)
    act_turned, upper_by, gated_by = pl.pallas_call(
        unpack_kernel,
        in_specs=[vmem, anywhere, anywhere],
        out_shape=[sds((width, slots), BF16), sds((half, slots), F32), sds((half, slots), F32)],
        cost_estimate=pl.CostEstimate(
            flops=20 * half * slots, bytes_accessed=6 * slots * width, transcendentals=0
        ),
        compiler_params=pltpu.CompilerParams(vmem_limit_bytes=16 * 2**20),
    )(rows_act.reshape(slots, -1), before_late[-1], after_late[-1])
    spread = pl.pallas_call(
        spread_kernel,
        in_specs=[pl.BlockSpec(memory_space=pltpu.SMEM), vmem, vmem, pl.BlockSpec(memory_space=pl.ANY)]
        + [vmem] * planes,
        out_shape=sds((slots, hidden), BF16),
        scratch_shapes=[pltpu.VMEM((hidden, tops * tokens), BF16)],
        cost_estimate=pl.CostEstimate(
            flops=2 * slots * hidden * tops * tokens, bytes_accessed=8 * slots * hidden, transcendentals=0
        ),
        compiler_params=pltpu.CompilerParams(vmem_limit_bytes=60 * 2**20),
    )(z.reshape(1), key, ids, upper_by, *act_pieces)
    both = pl.pallas_call(
        scale_kernel,
        in_specs=[vmem, vmem, vmem, anywhere],
        out_shape=sds((2 * half, slots), BF16),
        cost_estimate=pl.CostEstimate(flops=4 * half * slots, bytes_accessed=20 * half * slots, transcendentals=0),
        compiler_params=pltpu.CompilerParams(vmem_limit_bytes=16 * 2**20),
    )(total, upper_by, gated_by, spread)
    gathered = lax.all_gather(both, "gy", axis=0)
    rows_hidden = lax.all_to_all(spread.reshape(experts, MOST, -1), GX, 0, 0, tiled=True)
    down_t = lax.dot_general(
        rows_grad, rows_hidden.reshape(slots, hidden), (((0,), (0,)), ((), ())), preferred_element_type=F32
    )
    grad_gate, grad_up = final_grads(act_turned, gathered)
    return (grad_gate[None], grad_up[None], down_t.astype(BF16).T[None])


def solution(mesh):
    torus = Mesh(mesh.devices.reshape(4, 4, 2, mesh.shape["gy"]), ("gx_0", "gx_1", "gx_2", "gy"))
    return jax.shard_map(
        on_device,
        mesh=torus,
        in_specs=(
            P(GX, "gy"),
            P(GX, "gy"),
            P(GX, None, "gy"),
            P(GX, None, "gy"),
            P(GX, None),
            P(GX, None),
            P(GX, None, "gy"),
        ),
        out_specs=(P(GX, "gy", None), P(GX, "gy", None), P(GX, None, "gy")),
        check_vma=False,
    )
```

```python
import jax
import jax.numpy as jnp
from jax import lax
from jax.experimental import pallas as pl
from jax.experimental.pallas import tpu as pltpu
from jax.sharding import Mesh
from jax.sharding import PartitionSpec as P

MOST = 48
GX = ("gx_0", "gx_1", "gx_2")
F32 = jnp.float32
BF16 = jnp.bfloat16


def nt_dot(left, right):
    return lax.dot_general(left, right, (((1,), (1,)), ((), ())), preferred_element_type=F32)


def placing(key_ref, e):
    rank = lax.broadcasted_iota(jnp.int32, (MOST, key_ref.shape[1]), 0)
    return key_ref[pl.ds(e, 1), :] == rank


def picking(place, ids_ref, e):
    chosen = [
        place * jnp.where(ids_ref[pl.ds(k, 1), :] == e, 1.0, 0.0) for k in range(ids_ref.shape[0])
    ]
    return jnp.concatenate(chosen, axis=1)


def pack_kernel(
    ids_hbm, weight_hbm, gate_hbm, up_hbm, grad_hbm, act_out, rows_out, key_ref, both_ref,
    ids_ref, weight_ref, gate_ref, up_ref, grad_ref, share_ref, sems,
):
    pairs = (
        (ids_hbm, ids_ref),
        (weight_hbm, weight_ref),
        (gate_hbm, gate_ref),
        (up_hbm, up_ref),
        (grad_hbm, grad_ref),
    )
    copies = [pltpu.make_async_copy(src, dst, sems.at[i]) for i, (src, dst) in enumerate(pairs)]
    for copy in copies:
        copy.start()
    copies[0].wait()
    copies[1].wait()
    experts, tokens = key_ref.shape
    tops = ids_ref.shape[0]
    half = gate_ref.shape[1]
    expert_at = lax.broadcasted_iota(jnp.int32, (experts, tokens), 0)
    named = jnp.zeros((experts, tokens), F32)
    share = jnp.zeros((experts, tokens), F32)
    for k in range(tops):
        hit = ids_ref[pl.ds(k, 1), :] == expert_at
        named = named + jnp.where(hit, 1.0, 0.0)
        share = share + jnp.where(hit, weight_ref[pl.ds(k, 1), :], 0.0)
    before = (
        lax.broadcasted_iota(jnp.int32, (tokens, tokens), 0)
        < lax.broadcasted_iota(jnp.int32, (tokens, tokens), 1)
    ).astype(F32)
    earlier = jnp.dot(named.astype(BF16), before.astype(BF16), preferred_element_type=F32)
    key_ref[...] = jnp.where(named > 0.5, earlier.astype(jnp.int32), -1)
    share_ref[...] = share
    copies[2].wait()
    copies[3].wait()
    for k in range(tops):
        at = slice(tokens * k, tokens * (k + 1))
        both_ref[:half, at] = gate_ref[k]
        both_ref[half:, at] = up_ref[k]
        gate = gate_ref[k].astype(F32)
        sig = 1.0 / (1.0 + jnp.exp(-gate))
        act_out[:, at] = (gate * sig * up_ref[k].astype(F32)).astype(BF16)
    copies[4].wait()
    group = 4

    def step(at, carry):
        places, scales = [], []
        for i in range(group):
            e = at * group + i
            mine = placing(key_ref, e)
            places.append(jnp.where(mine, 1.0, 0.0))
            scales.append(jnp.sum(jnp.where(mine, share_ref[pl.ds(e, 1), :], 0.0), axis=1, keepdims=True))
        place = jnp.concatenate(places, axis=0).astype(BF16)
        scale = jnp.concatenate(scales, axis=0)
        rows = pl.ds(pl.multiple_of(at * (group * MOST), group * MOST), group * MOST)
        rows_out[rows, :] = (nt_dot(place, grad_ref[...]) * scale).astype(BF16)
        return carry

    lax.fori_loop(0, experts // group, step, 0)


def place_kernel(key_ref, ids_ref, both_ref, values_ref, sums_ref, out_ref):
    group = 4
    both = both_ref.shape[0]

    def step(at, carry):
        places, picks = [], []
        for i in range(group):
            e = at * group + i
            places.append(jnp.where(placing(key_ref, e), 1.0, 0.0))
            picks.append(picking(places[-1], ids_ref, e))
        rows = pl.ds(pl.multiple_of(at * (group * MOST), group * MOST), group * MOST)
        place = jnp.concatenate(places, axis=0).astype(BF16)
        pick = jnp.concatenate(picks, axis=0).astype(BF16)
        out_ref[rows, :both] = nt_dot(pick, both_ref[...]).astype(BF16)
        out_ref[rows, both:] = nt_dot(place, values_ref[...]).astype(BF16)
        return carry

    lax.fori_loop(0, key_ref.shape[0] // group, step, 0)


def spread_kernel(at_ref, key_ref, ids_ref, after_ref, *refs):
    pieces, out_ref, values_ref = refs[:-2], refs[-2], refs[-1]
    group = 4
    share = pieces[0].shape[0]
    for r, piece in enumerate(pieces):
        plane = lax.rem(at_ref[0] + r, len(pieces))
        values_ref[pl.ds(pl.multiple_of(plane * share, share), share), :] = piece[...]

    def step(at, carry):
        picks = []
        for i in range(group):
            e = at * group + i
            picks.append(picking(jnp.where(placing(key_ref, e), 1.0, 0.0), ids_ref, e))
        rows = pl.ds(pl.multiple_of(at * (group * MOST), group * MOST), group * MOST)
        pick = jnp.concatenate(picks, axis=0).astype(BF16)
        out_ref[rows, :] = nt_dot(pick, values_ref[...]).astype(BF16)
        return carry

    lax.fori_loop(0, key_ref.shape[0] // group, step, 0)


def weight_kernel(weight_ref, ahead_ref, behind_ref, out_ref):
    out_ref[...] = weight_ref[...].astype(F32).T.astype(BF16)


def unpack_kernel(rows_ref, ahead_ref, behind_ref, act_ref, upper_ref, gated_ref):
    half = upper_ref.shape[0]
    act_ref[...] = rows_ref[:, 2 * half :].astype(F32).T.astype(BF16)
    both = rows_ref[:, : 2 * half].astype(F32).T
    gate = both[:half]
    up = both[half:]
    sig = 1.0 / (1.0 + jnp.exp(-gate))
    upper_ref[...] = gate * sig
    gated_ref[...] = up * sig * (1.0 + gate * (1.0 - sig))


def scale_kernel(total_ref, upper_ref, gated_ref, out_ref):
    half = total_ref.shape[0]
    total = total_ref[...].astype(F32)
    out_ref[:half, :] = (total * gated_ref[...]).astype(BF16)
    out_ref[half:, :] = (total * upper_ref[...]).astype(BF16)


def final_kernel(act_ref, both_ref, gate_out, up_out):
    count, both, slots = both_ref.shape
    half = both // 2
    gate_out[...] = nt_dot(act_ref[...], both_ref[:, :half, :].reshape(count * half, slots)).astype(BF16)
    up_out[...] = nt_dot(act_ref[...], both_ref[:, half:, :].reshape(count * half, slots)).astype(BF16)


def final_grads(act_turned, gathered):
    width, slots = act_turned.shape
    planes, both, _ = gathered.shape
    group = 2
    spec = pl.BlockSpec((width, group * both // 2), lambda i: (0, i))
    shape = jax.ShapeDtypeStruct((width, planes * both // 2), BF16)
    return pl.pallas_call(
        final_kernel,
        grid=(planes // group,),
        in_specs=[
            pl.BlockSpec((width, slots), lambda i: (0, 0)),
            pl.BlockSpec((group, both, slots), lambda i: (i, 0, 0)),
        ],
        out_specs=[spec, spec],
        out_shape=[shape, shape],
        cost_estimate=pl.CostEstimate(
            flops=2 * width * slots * planes * both, bytes_accessed=2 * slots * planes * both, transcendentals=0
        ),
        compiler_params=pltpu.CompilerParams(vmem_limit_bytes=59 * 2**20),
    )(act_turned, gathered)


def hold_kernel(value_ref, after_ref, out_ref):
    out_ref[...] = value_ref[...]


def hold(value, after):
    return pl.pallas_call(
        hold_kernel,
        in_specs=[pl.BlockSpec(memory_space=pltpu.VMEM), pl.BlockSpec(memory_space=pl.ANY)],
        out_shape=jax.ShapeDtypeStruct(value.shape, value.dtype),
        cost_estimate=pl.CostEstimate(flops=0, bytes_accessed=4 * value.size, transcendentals=0),
        compiler_params=pltpu.CompilerParams(vmem_limit_bytes=4 * 2**20),
    )(value, after)


def ring_rounds(ahead, behind, axis, rounds, both_ways):
    count = lax.axis_size(axis)
    plus = [(i, (i + 1) % count) for i in range(count)]
    minus = [(i, (i - 1) % count) for i in range(count)]
    before, after = [], []
    for s in range(rounds):
        ahead = lax.ppermute(ahead, axis, plus)
        before.append(ahead)
        if s < both_ways:
            behind = lax.ppermute(behind, axis, minus)
            after.append(behind)
    return before, after


def on_device(activations, out_grad, saved_gate, saved_up, route_ids, route_weight, down_weight):
    experts = lax.axis_size(GX)
    planes = lax.axis_size("gy")
    z = lax.axis_index("gy")
    tokens, width = activations.shape
    tops = route_ids.shape[1]
    slots = experts * MOST
    half = saved_gate.shape[2]
    hidden = down_weight.shape[1]
    sds = jax.ShapeDtypeStruct
    ids = route_ids.T
    gate = jnp.transpose(saved_gate, (1, 2, 0))
    up = jnp.transpose(saved_up, (1, 2, 0))
    hbm = pl.BlockSpec(memory_space=pltpu.MemorySpace.HBM)
    act_share, routes, key, gate_up = pl.pallas_call(
        pack_kernel,
        in_specs=[hbm] * 5,
        out_shape=[
            sds((half, tops * tokens), BF16),
            sds((slots, width), BF16),
            sds((experts, tokens), jnp.int32),
            sds((2 * half, tops * tokens), BF16),
        ],
        scratch_shapes=[
            pltpu.VMEM((tops, tokens), jnp.int32),
            pltpu.VMEM((tops, tokens), F32),
            pltpu.VMEM((tops, half, tokens), BF16),
            pltpu.VMEM((tops, half, tokens), BF16),
            pltpu.VMEM((width, tokens), BF16),
            pltpu.VMEM((experts, tokens), F32),
            pltpu.SemaphoreType.DMA((5,)),
        ],
        cost_estimate=pl.CostEstimate(
            flops=2 * slots * tokens * (width + 16 * half), bytes_accessed=4 * slots * width, transcendentals=0
        ),
        compiler_params=pltpu.CompilerParams(vmem_limit_bytes=60 * 2**20),
    )(ids, route_weight.T, gate, up, out_grad.T)
    early = 2
    before, after = ring_rounds(act_share, act_share, "gy", early, early)
    turned = pl.pallas_call(
        weight_kernel,
        in_specs=[pl.BlockSpec(memory_space=pltpu.VMEM)] + [pl.BlockSpec(memory_space=pl.ANY)] * 2,
        out_shape=sds((hidden, width), BF16),
        cost_estimate=pl.CostEstimate(flops=0, bytes_accessed=6 * hidden * width, transcendentals=0),
        compiler_params=pltpu.CompilerParams(vmem_limit_bytes=16 * 2**20),
    )(down_weight[0].T, before[-1], after[-1])
    rows_grad = lax.all_to_all(routes.reshape(experts, MOST, -1), GX, 0, 0, tiled=True).reshape(slots, -1)
    sums = nt_dot(turned, rows_grad).astype(BF16)
    total = lax.psum_scatter(sums, "gy", scatter_dimension=0, tiled=True)
    packed = pl.pallas_call(
        place_kernel,
        in_specs=[pl.BlockSpec(memory_space=pltpu.VMEM)] * 4 + [pl.BlockSpec(memory_space=pl.ANY)],
        out_shape=sds((slots, 2 * half + width), BF16),
        cost_estimate=pl.CostEstimate(
            flops=2 * slots * tokens * (width + 16 * half), bytes_accessed=2 * slots * width, transcendentals=0
        ),
        compiler_params=pltpu.CompilerParams(vmem_limit_bytes=16 * 2**20),
    )(key, ids, gate_up, activations.T, sums)
    late = planes // 2 - early
    before_late, after_late = ring_rounds(hold(before[-1], packed), after[-1], "gy", late, late - 1)
    act_pieces = [act_share] + after + after_late + (before + before_late)[::-1]
    rows_act = lax.all_to_all(packed.reshape(experts, MOST, -1), GX, 0, 0, tiled=True)
    vmem = pl.BlockSpec(memory_space=pltpu.VMEM)
    anywhere = pl.BlockSpec(memory_space=pl.ANY)
    act_turned, upper_by, gated_by = pl.pallas_call(
        unpack_kernel,
        in_specs=[vmem, anywhere, anywhere],
        out_shape=[sds((width, slots), BF16), sds((half, slots), F32), sds((half, slots), F32)],
        cost_estimate=pl.CostEstimate(
            flops=20 * half * slots, bytes_accessed=6 * slots * width, transcendentals=0
        ),
        compiler_params=pltpu.CompilerParams(vmem_limit_bytes=16 * 2**20),
    )(rows_act.reshape(slots, -1), before_late[-1], after_late[-1])
    both = pl.pallas_call(
        scale_kernel,
        in_specs=[vmem, vmem, vmem],
        out_shape=sds((2 * half, slots), BF16),
        cost_estimate=pl.CostEstimate(flops=4 * half * slots, bytes_accessed=20 * half * slots, transcendentals=0),
        compiler_params=pltpu.CompilerParams(vmem_limit_bytes=60 * 2**20),
    )(total, upper_by, gated_by)
    gathered = lax.all_gather(both, "gy", axis=0)
    spread = pl.pallas_call(
        spread_kernel,
        in_specs=[pl.BlockSpec(memory_space=pltpu.SMEM), vmem, vmem, pl.BlockSpec(memory_space=pl.ANY)]
        + [vmem] * planes,
        out_shape=sds((slots, hidden), BF16),
        scratch_shapes=[pltpu.VMEM((hidden, tops * tokens), BF16)],
        cost_estimate=pl.CostEstimate(
            flops=2 * slots * hidden * tops * tokens, bytes_accessed=8 * slots * hidden, transcendentals=0
        ),
        compiler_params=pltpu.CompilerParams(vmem_limit_bytes=60 * 2**20),
    )(z.reshape(1), key, ids, both, *act_pieces)
    rows_hidden = lax.all_to_all(spread.reshape(experts, MOST, -1), GX, 0, 0, tiled=True)
    down_t = lax.dot_general(
        rows_grad, rows_hidden.reshape(slots, hidden), (((0,), (0,)), ((), ())), preferred_element_type=F32
    )
    grad_gate, grad_up = final_grads(act_turned, gathered)
    return (grad_gate[None], grad_up[None], down_t.astype(BF16).T[None])


def solution(mesh):
    torus = Mesh(mesh.devices.reshape(4, 4, 2, mesh.shape["gy"]), ("gx_0", "gx_1", "gx_2", "gy"))
    return jax.shard_map(
        on_device,
        mesh=torus,
        in_specs=(
            P(GX, "gy"),
            P(GX, "gy"),
            P(GX, None, "gy"),
            P(GX, None, "gy"),
            P(GX, None),
            P(GX, None),
            P(GX, None, "gy"),
        ),
        out_specs=(P(GX, "gy", None), P(GX, "gy", None), P(GX, None, "gy")),
        check_vma=False,
    )
```

```python
import jax
import jax.numpy as jnp
from jax import lax
from jax.experimental import pallas as pl
from jax.experimental.pallas import tpu as pltpu
from jax.sharding import Mesh
from jax.sharding import PartitionSpec as P

MOST = 48
GX = ("gx_0", "gx_1", "gx_2")
F32 = jnp.float32
BF16 = jnp.bfloat16


def nt_dot(left, right):
    return lax.dot_general(left, right, (((1,), (1,)), ((), ())), preferred_element_type=F32)


def placing(key_ref, e):
    rank = lax.broadcasted_iota(jnp.int32, (MOST, key_ref.shape[1]), 0)
    return key_ref[pl.ds(e, 1), :] == rank


def picking(place, ids_ref, e):
    chosen = [
        place * jnp.where(ids_ref[pl.ds(k, 1), :] == e, 1.0, 0.0) for k in range(ids_ref.shape[0])
    ]
    return jnp.concatenate(chosen, axis=1)


def pack_kernel(
    ids_hbm, weight_hbm, gate_hbm, up_hbm, grad_hbm, act_out, rows_out, key_ref, both_ref,
    ids_ref, weight_ref, gate_ref, up_ref, grad_ref, share_ref, sems,
):
    pairs = (
        (ids_hbm, ids_ref),
        (weight_hbm, weight_ref),
        (gate_hbm, gate_ref),
        (up_hbm, up_ref),
        (grad_hbm, grad_ref),
    )
    copies = [pltpu.make_async_copy(src, dst, sems.at[i]) for i, (src, dst) in enumerate(pairs)]
    for copy in copies:
        copy.start()
    copies[0].wait()
    copies[1].wait()
    experts, tokens = key_ref.shape
    tops = ids_ref.shape[0]
    half = gate_ref.shape[1]
    expert_at = lax.broadcasted_iota(jnp.int32, (experts, tokens), 0)
    named = jnp.zeros((experts, tokens), F32)
    share = jnp.zeros((experts, tokens), F32)
    for k in range(tops):
        hit = ids_ref[pl.ds(k, 1), :] == expert_at
        named = named + jnp.where(hit, 1.0, 0.0)
        share = share + jnp.where(hit, weight_ref[pl.ds(k, 1), :], 0.0)
    before = (
        lax.broadcasted_iota(jnp.int32, (tokens, tokens), 0)
        < lax.broadcasted_iota(jnp.int32, (tokens, tokens), 1)
    ).astype(F32)
    earlier = jnp.dot(named.astype(BF16), before.astype(BF16), preferred_element_type=F32)
    key_ref[...] = jnp.where(named > 0.5, earlier.astype(jnp.int32), -1)
    share_ref[...] = share
    copies[2].wait()
    copies[3].wait()
    for k in range(tops):
        at = slice(tokens * k, tokens * (k + 1))
        both_ref[:half, at] = gate_ref[k]
        both_ref[half:, at] = up_ref[k]
        gate = gate_ref[k].astype(F32)
        sig = 1.0 / (1.0 + jnp.exp(-gate))
        act_out[:, at] = (gate * sig * up_ref[k].astype(F32)).astype(BF16)
    copies[4].wait()
    group = 4

    def step(at, carry):
        places, scales = [], []
        for i in range(group):
            e = at * group + i
            mine = placing(key_ref, e)
            places.append(jnp.where(mine, 1.0, 0.0))
            scales.append(jnp.sum(jnp.where(mine, share_ref[pl.ds(e, 1), :], 0.0), axis=1, keepdims=True))
        place = jnp.concatenate(places, axis=0).astype(BF16)
        scale = jnp.concatenate(scales, axis=0)
        rows = pl.ds(pl.multiple_of(at * (group * MOST), group * MOST), group * MOST)
        rows_out[rows, :] = (nt_dot(place, grad_ref[...]) * scale).astype(BF16)
        return carry

    lax.fori_loop(0, experts // group, step, 0)


def place_kernel(key_ref, ids_ref, both_ref, values_ref, rows_ref, sums_ref, out_ref, kept_ref):
    kept_ref[...] = rows_ref[...]
    group = 4
    both = both_ref.shape[0]

    def step(at, carry):
        places, picks = [], []
        for i in range(group):
            e = at * group + i
            places.append(jnp.where(placing(key_ref, e), 1.0, 0.0))
            picks.append(picking(places[-1], ids_ref, e))
        rows = pl.ds(pl.multiple_of(at * (group * MOST), group * MOST), group * MOST)
        place = jnp.concatenate(places, axis=0).astype(BF16)
        pick = jnp.concatenate(picks, axis=0).astype(BF16)
        out_ref[rows, :both] = nt_dot(pick, both_ref[...]).astype(BF16)
        out_ref[rows, both:] = nt_dot(place, values_ref[...]).astype(BF16)
        return carry

    lax.fori_loop(0, key_ref.shape[0] // group, step, 0)


def spread_kernel(at_ref, key_ref, ids_ref, after_ref, *refs):
    pieces, out_ref, values_ref = refs[:-2], refs[-2], refs[-1]
    group = 4
    share = pieces[0].shape[0]
    for r, piece in enumerate(pieces):
        plane = lax.rem(at_ref[0] + r, len(pieces))
        values_ref[pl.ds(pl.multiple_of(plane * share, share), share), :] = piece[...]

    def step(at, carry):
        picks = []
        for i in range(group):
            e = at * group + i
            picks.append(picking(jnp.where(placing(key_ref, e), 1.0, 0.0), ids_ref, e))
        rows = pl.ds(pl.multiple_of(at * (group * MOST), group * MOST), group * MOST)
        pick = jnp.concatenate(picks, axis=0).astype(BF16)
        out_ref[rows, :] = nt_dot(pick, values_ref[...]).astype(BF16)
        return carry

    lax.fori_loop(0, key_ref.shape[0] // group, step, 0)


def weight_kernel(weight_ref, ahead_ref, behind_ref, out_ref):
    out_ref[...] = weight_ref[...].astype(F32).T.astype(BF16)


def unpack_kernel(rows_ref, ahead_ref, behind_ref, act_ref, upper_ref, gated_ref):
    half = upper_ref.shape[0]
    act_ref[...] = rows_ref[:, 2 * half :].astype(F32).T.astype(BF16)
    both = rows_ref[:, : 2 * half].astype(F32).T
    gate = both[:half]
    up = both[half:]
    sig = 1.0 / (1.0 + jnp.exp(-gate))
    upper_ref[...] = gate * sig
    gated_ref[...] = up * sig * (1.0 + gate * (1.0 - sig))


def scale_kernel(total_ref, upper_ref, gated_ref, out_ref):
    half = total_ref.shape[0]
    total = total_ref[...].astype(F32)
    out_ref[:half, :] = (total * gated_ref[...]).astype(BF16)
    out_ref[half:, :] = (total * upper_ref[...]).astype(BF16)


def final_kernel(act_ref, both_ref, gate_out, up_out):
    count, half, slots = both_ref.shape
    value = nt_dot(act_ref[...], both_ref[...].reshape(count * half, slots)).astype(BF16)

    @pl.when(pl.program_id(0) % 2 == 0)
    def _():
        gate_out[...] = value

    @pl.when(pl.program_id(0) % 2 == 1)
    def _():
        up_out[...] = value


def final_grads(act_turned, gathered):
    width, slots = act_turned.shape
    planes, both, _ = gathered.shape
    group = 4
    spec = pl.BlockSpec((width, group * both // 2), lambda i: (0, i // 2))
    shape = jax.ShapeDtypeStruct((width, planes * both // 2), BF16)
    return pl.pallas_call(
        final_kernel,
        grid=(2 * planes // group,),
        in_specs=[
            pl.BlockSpec((width, slots), lambda i: (0, 0)),
            pl.BlockSpec((group, both // 2, slots), lambda i: (i // 2, i % 2, 0)),
        ],
        out_specs=[spec, spec],
        out_shape=[shape, shape],
        cost_estimate=pl.CostEstimate(
            flops=2 * width * slots * planes * both, bytes_accessed=2 * slots * planes * both, transcendentals=0
        ),
        compiler_params=pltpu.CompilerParams(vmem_limit_bytes=59 * 2**20),
    )(act_turned, gathered)


def hold_kernel(value_ref, after_ref, out_ref):
    out_ref[...] = value_ref[...]


def hold(value, after):
    return pl.pallas_call(
        hold_kernel,
        in_specs=[pl.BlockSpec(memory_space=pltpu.VMEM), pl.BlockSpec(memory_space=pl.ANY)],
        out_shape=jax.ShapeDtypeStruct(value.shape, value.dtype),
        cost_estimate=pl.CostEstimate(flops=0, bytes_accessed=4 * value.size, transcendentals=0),
        compiler_params=pltpu.CompilerParams(vmem_limit_bytes=4 * 2**20),
    )(value, after)


def ring_rounds(ahead, behind, axis, rounds, both_ways):
    count = lax.axis_size(axis)
    plus = [(i, (i + 1) % count) for i in range(count)]
    minus = [(i, (i - 1) % count) for i in range(count)]
    before, after = [], []
    for s in range(rounds):
        ahead = lax.ppermute(ahead, axis, plus)
        before.append(ahead)
        if s < both_ways:
            behind = lax.ppermute(behind, axis, minus)
            after.append(behind)
    return before, after


def on_device(activations, out_grad, saved_gate, saved_up, route_ids, route_weight, down_weight):
    experts = lax.axis_size(GX)
    planes = lax.axis_size("gy")
    z = lax.axis_index("gy")
    tokens, width = activations.shape
    tops = route_ids.shape[1]
    slots = experts * MOST
    half = saved_gate.shape[2]
    hidden = down_weight.shape[1]
    sds = jax.ShapeDtypeStruct
    ids = route_ids.T
    gate = jnp.transpose(saved_gate, (1, 2, 0))
    up = jnp.transpose(saved_up, (1, 2, 0))
    hbm = pl.BlockSpec(memory_space=pltpu.MemorySpace.HBM)
    act_share, routes, key, gate_up = pl.pallas_call(
        pack_kernel,
        in_specs=[hbm] * 5,
        out_shape=[
            sds((half, tops * tokens), BF16),
            sds((slots, width), BF16),
            sds((experts, tokens), jnp.int32),
            sds((2 * half, tops * tokens), BF16),
        ],
        scratch_shapes=[
            pltpu.VMEM((tops, tokens), jnp.int32),
            pltpu.VMEM((tops, tokens), F32),
            pltpu.VMEM((tops, half, tokens), BF16),
            pltpu.VMEM((tops, half, tokens), BF16),
            pltpu.VMEM((width, tokens), BF16),
            pltpu.VMEM((experts, tokens), F32),
            pltpu.SemaphoreType.DMA((5,)),
        ],
        cost_estimate=pl.CostEstimate(
            flops=2 * slots * tokens * (width + 16 * half), bytes_accessed=4 * slots * width, transcendentals=0
        ),
        compiler_params=pltpu.CompilerParams(vmem_limit_bytes=60 * 2**20),
    )(ids, route_weight.T, gate, up, out_grad.T)
    early = 2
    before, after = ring_rounds(act_share, act_share, "gy", early, early)
    turned = pl.pallas_call(
        weight_kernel,
        in_specs=[pl.BlockSpec(memory_space=pltpu.VMEM)] + [pl.BlockSpec(memory_space=pl.ANY)] * 2,
        out_shape=sds((hidden, width), BF16),
        cost_estimate=pl.CostEstimate(flops=0, bytes_accessed=6 * hidden * width, transcendentals=0),
        compiler_params=pltpu.CompilerParams(vmem_limit_bytes=16 * 2**20),
    )(down_weight[0].T, before[-1], after[-1])
    rows_grad = lax.all_to_all(routes.reshape(experts, MOST, -1), GX, 0, 0, tiled=True).reshape(slots, -1)
    sums = nt_dot(turned, rows_grad).astype(BF16)
    total = lax.psum_scatter(sums, "gy", scatter_dimension=0, tiled=True)
    packed, rows_kept = pl.pallas_call(
        place_kernel,
        in_specs=[pl.BlockSpec(memory_space=pltpu.VMEM)] * 5 + [pl.BlockSpec(memory_space=pl.ANY)],
        out_shape=[sds((slots, 2 * half + width), BF16), sds((slots, width), BF16)],
        cost_estimate=pl.CostEstimate(
            flops=2 * slots * tokens * (width + 16 * half), bytes_accessed=2 * slots * width, transcendentals=0
        ),
        compiler_params=pltpu.CompilerParams(vmem_limit_bytes=16 * 2**20),
    )(key, ids, gate_up, activations.T, rows_grad, sums[:16, :128])
    late = planes // 2 - early
    before_late, after_late = ring_rounds(hold(before[-1], packed), after[-1], "gy", late, late - 1)
    act_pieces = [act_share] + after + after_late + (before + before_late)[::-1]
    rows_act = lax.all_to_all(packed.reshape(experts, MOST, -1), GX, 0, 0, tiled=True)
    vmem = pl.BlockSpec(memory_space=pltpu.VMEM)
    anywhere = pl.BlockSpec(memory_space=pl.ANY)
    act_turned, upper_by, gated_by = pl.pallas_call(
        unpack_kernel,
        in_specs=[vmem, anywhere, anywhere],
        out_shape=[sds((width, slots), BF16), sds((half, slots), F32), sds((half, slots), F32)],
        cost_estimate=pl.CostEstimate(
            flops=20 * half * slots, bytes_accessed=6 * slots * width, transcendentals=0
        ),
        compiler_params=pltpu.CompilerParams(vmem_limit_bytes=60 * 2**20),
    )(rows_act.reshape(slots, -1), before_late[-1], after_late[-1])
    both = pl.pallas_call(
        scale_kernel,
        in_specs=[vmem, vmem, vmem],
        out_shape=sds((2 * half, slots), BF16),
        cost_estimate=pl.CostEstimate(flops=4 * half * slots, bytes_accessed=20 * half * slots, transcendentals=0),
        compiler_params=pltpu.CompilerParams(vmem_limit_bytes=60 * 2**20),
    )(total, upper_by, gated_by)
    gathered = lax.all_gather(both, "gy", axis=0)
    spread = pl.pallas_call(
        spread_kernel,
        in_specs=[pl.BlockSpec(memory_space=pltpu.SMEM), vmem, vmem, pl.BlockSpec(memory_space=pl.ANY)]
        + [vmem] * planes,
        out_shape=sds((slots, hidden), BF16),
        scratch_shapes=[pltpu.VMEM((hidden, tops * tokens), BF16)],
        cost_estimate=pl.CostEstimate(
            flops=2 * slots * hidden * tops * tokens, bytes_accessed=8 * slots * hidden, transcendentals=0
        ),
        compiler_params=pltpu.CompilerParams(vmem_limit_bytes=60 * 2**20),
    )(z.reshape(1), key, ids, both, *act_pieces)
    rows_hidden = lax.all_to_all(spread.reshape(experts, MOST, -1), GX, 0, 0, tiled=True)
    down_t = lax.dot_general(
        rows_kept, rows_hidden.reshape(slots, hidden), (((0,), (0,)), ((), ())), preferred_element_type=F32
    )
    grad_gate, grad_up = final_grads(act_turned, gathered)
    return (grad_gate[None], grad_up[None], down_t.astype(BF16).T[None])


def solution(mesh):
    torus = Mesh(mesh.devices.reshape(4, 4, 2, mesh.shape["gy"]), ("gx_0", "gx_1", "gx_2", "gy"))
    return jax.shard_map(
        on_device,
        mesh=torus,
        in_specs=(
            P(GX, "gy"),
            P(GX, "gy"),
            P(GX, None, "gy"),
            P(GX, None, "gy"),
            P(GX, None),
            P(GX, None),
            P(GX, None, "gy"),
        ),
        out_specs=(P(GX, "gy", None), P(GX, "gy", None), P(GX, None, "gy")),
        check_vma=False,
    )
```

```python
import jax
import jax.numpy as jnp
from jax import lax
from jax.experimental import pallas as pl
from jax.experimental.pallas import tpu as pltpu
from jax.sharding import Mesh
from jax.sharding import PartitionSpec as P

MOST = 48
GX = ("gx_0", "gx_1", "gx_2")
F32 = jnp.float32
BF16 = jnp.bfloat16


def nt_dot(left, right):
    return lax.dot_general(left, right, (((1,), (1,)), ((), ())), preferred_element_type=F32)


def placing(key_ref, e):
    rank = lax.broadcasted_iota(jnp.int32, (MOST, key_ref.shape[1]), 0)
    return key_ref[pl.ds(e, 1), :] == rank


def picking(place, ids_ref, e):
    chosen = [
        place * jnp.where(ids_ref[pl.ds(k, 1), :] == e, 1.0, 0.0) for k in range(ids_ref.shape[0])
    ]
    return jnp.concatenate(chosen, axis=1)


def pack_kernel(
    ids_hbm, weight_hbm, gate_hbm, up_hbm, grad_hbm, act_out, rows_out, key_ref, both_ref,
    ids_ref, weight_ref, gate_ref, up_ref, grad_ref, share_ref, sems,
):
    pairs = (
        (ids_hbm, ids_ref),
        (weight_hbm, weight_ref),
        (gate_hbm, gate_ref),
        (up_hbm, up_ref),
        (grad_hbm, grad_ref),
    )
    copies = [pltpu.make_async_copy(src, dst, sems.at[i]) for i, (src, dst) in enumerate(pairs)]
    for copy in copies:
        copy.start()
    copies[0].wait()
    copies[1].wait()
    experts, tokens = key_ref.shape
    tops = ids_ref.shape[0]
    half = gate_ref.shape[1]
    expert_at = lax.broadcasted_iota(jnp.int32, (experts, tokens), 0)
    named = jnp.zeros((experts, tokens), F32)
    share = jnp.zeros((experts, tokens), F32)
    for k in range(tops):
        hit = ids_ref[pl.ds(k, 1), :] == expert_at
        named = named + jnp.where(hit, 1.0, 0.0)
        share = share + jnp.where(hit, weight_ref[pl.ds(k, 1), :], 0.0)
    before = (
        lax.broadcasted_iota(jnp.int32, (tokens, tokens), 0)
        < lax.broadcasted_iota(jnp.int32, (tokens, tokens), 1)
    ).astype(F32)
    earlier = jnp.dot(named.astype(BF16), before.astype(BF16), preferred_element_type=F32)
    key_ref[...] = jnp.where(named > 0.5, earlier.astype(jnp.int32), -1)
    share_ref[...] = share
    copies[2].wait()
    copies[3].wait()
    for k in range(tops):
        at = slice(tokens * k, tokens * (k + 1))
        both_ref[:half, at] = gate_ref[k]
        both_ref[half:, at] = up_ref[k]
        gate = gate_ref[k].astype(F32)
        sig = 1.0 / (1.0 + jnp.exp(-gate))
        act_out[:, at] = (gate * sig * up_ref[k].astype(F32)).astype(BF16)
    copies[4].wait()
    group = 4

    def step(at, carry):
        places, scales = [], []
        for i in range(group):
            e = at * group + i
            mine = placing(key_ref, e)
            places.append(jnp.where(mine, 1.0, 0.0))
            scales.append(jnp.sum(jnp.where(mine, share_ref[pl.ds(e, 1), :], 0.0), axis=1, keepdims=True))
        place = jnp.concatenate(places, axis=0).astype(BF16)
        scale = jnp.concatenate(scales, axis=0)
        rows = pl.ds(pl.multiple_of(at * (group * MOST), group * MOST), group * MOST)
        rows_out[rows, :] = (nt_dot(place, grad_ref[...]) * scale).astype(BF16)
        return carry

    lax.fori_loop(0, experts // group, step, 0)


def place_kernel(key_ref, ids_ref, both_ref, values_ref, rows_ref, sums_ref, out_ref, kept_ref):
    kept_ref[...] = rows_ref[...]
    group = 4
    both = both_ref.shape[0]

    def step(at, carry):
        places, picks = [], []
        for i in range(group):
            e = at * group + i
            places.append(jnp.where(placing(key_ref, e), 1.0, 0.0))
            picks.append(picking(places[-1], ids_ref, e))
        rows = pl.ds(pl.multiple_of(at * (group * MOST), group * MOST), group * MOST)
        place = jnp.concatenate(places, axis=0).astype(BF16)
        pick = jnp.concatenate(picks, axis=0).astype(BF16)
        out_ref[rows, :both] = nt_dot(pick, both_ref[...]).astype(BF16)
        out_ref[rows, both:] = nt_dot(place, values_ref[...]).astype(BF16)
        return carry

    lax.fori_loop(0, key_ref.shape[0] // group, step, 0)


def spread_kernel(at_ref, key_ref, ids_ref, after_ref, *refs):
    pieces, out_ref, values_ref = refs[:-2], refs[-2], refs[-1]
    group = 4
    share = pieces[0].shape[0]
    for r, piece in enumerate(pieces):
        plane = lax.rem(at_ref[0] + r, len(pieces))
        values_ref[pl.ds(pl.multiple_of(plane * share, share), share), :] = piece[...]

    def step(at, carry):
        picks = []
        for i in range(group):
            e = at * group + i
            picks.append(picking(jnp.where(placing(key_ref, e), 1.0, 0.0), ids_ref, e))
        rows = pl.ds(pl.multiple_of(at * (group * MOST), group * MOST), group * MOST)
        pick = jnp.concatenate(picks, axis=0).astype(BF16)
        out_ref[rows, :] = nt_dot(pick, values_ref[...]).astype(BF16)
        return carry

    lax.fori_loop(0, key_ref.shape[0] // group, step, 0)


def weight_kernel(weight_ref, ahead_ref, behind_ref, out_ref):
    out_ref[...] = weight_ref[...].astype(F32).T.astype(BF16)


def unpack_kernel(rows_ref, ahead_ref, behind_ref, act_ref, upper_ref, gated_ref):
    half = upper_ref.shape[0]
    act_ref[...] = rows_ref[:, 2 * half :].astype(F32).T.astype(BF16)
    both = rows_ref[:, : 2 * half].astype(F32).T
    gate = both[:half]
    up = both[half:]
    sig = 1.0 / (1.0 + jnp.exp(-gate))
    upper_ref[...] = gate * sig
    gated_ref[...] = up * sig * (1.0 + gate * (1.0 - sig))


def scale_kernel(total_ref, upper_ref, gated_ref, out_ref):
    half = total_ref.shape[0]
    total = total_ref[...].astype(F32)
    out_ref[:half, :] = (total * gated_ref[...]).astype(BF16)
    out_ref[half:, :] = (total * upper_ref[...]).astype(BF16)


def final_kernel(act_ref, both_ref, gate_out, up_out):
    count, both, slots = both_ref.shape
    half = both // 2
    gate_out[...] = nt_dot(act_ref[...], both_ref[:, :half, :].reshape(count * half, slots)).astype(BF16)
    up_out[...] = nt_dot(act_ref[...], both_ref[:, half:, :].reshape(count * half, slots)).astype(BF16)


def final_grads(act_turned, gathered):
    width, slots = act_turned.shape
    planes, both, _ = gathered.shape
    group = 4
    spec = pl.BlockSpec((width, group * both // 2), lambda i: (0, i))
    shape = jax.ShapeDtypeStruct((width, planes * both // 2), BF16)
    return pl.pallas_call(
        final_kernel,
        grid=(planes // group,),
        in_specs=[
            pl.BlockSpec((width, slots), lambda i: (0, 0)),
            pl.BlockSpec((group, both, slots), lambda i: (i, 0, 0)),
        ],
        out_specs=[spec, spec],
        out_shape=[shape, shape],
        cost_estimate=pl.CostEstimate(
            flops=2 * width * slots * planes * both, bytes_accessed=2 * slots * planes * both, transcendentals=0
        ),
        compiler_params=pltpu.CompilerParams(vmem_limit_bytes=59 * 2**20),
    )(act_turned, gathered)


def hold_kernel(value_ref, after_ref, out_ref):
    out_ref[...] = value_ref[...]


def hold(value, after):
    return pl.pallas_call(
        hold_kernel,
        in_specs=[pl.BlockSpec(memory_space=pltpu.VMEM), pl.BlockSpec(memory_space=pl.ANY)],
        out_shape=jax.ShapeDtypeStruct(value.shape, value.dtype),
        cost_estimate=pl.CostEstimate(flops=0, bytes_accessed=4 * value.size, transcendentals=0),
        compiler_params=pltpu.CompilerParams(vmem_limit_bytes=4 * 2**20),
    )(value, after)


def ring_rounds(ahead, behind, axis, rounds, both_ways):
    count = lax.axis_size(axis)
    plus = [(i, (i + 1) % count) for i in range(count)]
    minus = [(i, (i - 1) % count) for i in range(count)]
    before, after = [], []
    for s in range(rounds):
        ahead = lax.ppermute(ahead, axis, plus)
        before.append(ahead)
        if s < both_ways:
            behind = lax.ppermute(behind, axis, minus)
            after.append(behind)
    return before, after


def on_device(activations, out_grad, saved_gate, saved_up, route_ids, route_weight, down_weight):
    experts = lax.axis_size(GX)
    planes = lax.axis_size("gy")
    z = lax.axis_index("gy")
    tokens, width = activations.shape
    tops = route_ids.shape[1]
    slots = experts * MOST
    half = saved_gate.shape[2]
    hidden = down_weight.shape[1]
    sds = jax.ShapeDtypeStruct
    ids = route_ids.T
    gate = jnp.transpose(saved_gate, (1, 2, 0))
    up = jnp.transpose(saved_up, (1, 2, 0))
    hbm = pl.BlockSpec(memory_space=pltpu.MemorySpace.HBM)
    act_share, routes, key, gate_up = pl.pallas_call(
        pack_kernel,
        in_specs=[hbm] * 5,
        out_shape=[
            sds((half, tops * tokens), BF16),
            sds((slots, width), BF16),
            sds((experts, tokens), jnp.int32),
            sds((2 * half, tops * tokens), BF16),
        ],
        scratch_shapes=[
            pltpu.VMEM((tops, tokens), jnp.int32),
            pltpu.VMEM((tops, tokens), F32),
            pltpu.VMEM((tops, half, tokens), BF16),
            pltpu.VMEM((tops, half, tokens), BF16),
            pltpu.VMEM((width, tokens), BF16),
            pltpu.VMEM((experts, tokens), F32),
            pltpu.SemaphoreType.DMA((5,)),
        ],
        cost_estimate=pl.CostEstimate(
            flops=2 * slots * tokens * (width + 16 * half), bytes_accessed=4 * slots * width, transcendentals=0
        ),
        compiler_params=pltpu.CompilerParams(vmem_limit_bytes=60 * 2**20),
    )(ids, route_weight.T, gate, up, out_grad.T)
    early = 2
    before, after = ring_rounds(act_share, act_share, "gy", early, early)
    turned = pl.pallas_call(
        weight_kernel,
        in_specs=[pl.BlockSpec(memory_space=pltpu.VMEM)] + [pl.BlockSpec(memory_space=pl.ANY)] * 2,
        out_shape=sds((hidden, width), BF16),
        cost_estimate=pl.CostEstimate(flops=0, bytes_accessed=6 * hidden * width, transcendentals=0),
        compiler_params=pltpu.CompilerParams(vmem_limit_bytes=16 * 2**20),
    )(down_weight[0].T, before[-1], after[-1])
    rows_grad = lax.all_to_all(routes.reshape(experts, MOST, -1), GX, 0, 0, tiled=True).reshape(slots, -1)
    sums = nt_dot(turned, rows_grad).astype(BF16)
    total = lax.psum_scatter(sums, "gy", scatter_dimension=0, tiled=True)
    packed, rows_kept = pl.pallas_call(
        place_kernel,
        in_specs=[pl.BlockSpec(memory_space=pltpu.VMEM)] * 5 + [pl.BlockSpec(memory_space=pl.ANY)],
        out_shape=[sds((slots, 2 * half + width), BF16), sds((slots, width), BF16)],
        cost_estimate=pl.CostEstimate(
            flops=2 * slots * tokens * (width + 16 * half), bytes_accessed=2 * slots * width, transcendentals=0
        ),
        compiler_params=pltpu.CompilerParams(vmem_limit_bytes=16 * 2**20),
    )(key, ids, gate_up, activations.T, rows_grad, sums[:16, :128])
    late = planes // 2 - early
    before_late, after_late = ring_rounds(hold(before[-1], packed), after[-1], "gy", late, late - 1)
    act_pieces = [act_share] + after + after_late + (before + before_late)[::-1]
    rows_act = lax.all_to_all(packed.reshape(experts, MOST, -1), GX, 0, 0, tiled=True)
    vmem = pl.BlockSpec(memory_space=pltpu.VMEM)
    anywhere = pl.BlockSpec(memory_space=pl.ANY)
    act_turned, upper_by, gated_by = pl.pallas_call(
        unpack_kernel,
        in_specs=[vmem, anywhere, anywhere],
        out_shape=[sds((width, slots), BF16), sds((half, slots), F32), sds((half, slots), F32)],
        cost_estimate=pl.CostEstimate(
            flops=20 * half * slots, bytes_accessed=6 * slots * width, transcendentals=0
        ),
        compiler_params=pltpu.CompilerParams(vmem_limit_bytes=60 * 2**20),
    )(rows_act.reshape(slots, -1), before_late[-1], after_late[-1])
    both = pl.pallas_call(
        scale_kernel,
        in_specs=[vmem, vmem, vmem],
        out_shape=sds((2 * half, slots), BF16),
        cost_estimate=pl.CostEstimate(flops=4 * half * slots, bytes_accessed=20 * half * slots, transcendentals=0),
        compiler_params=pltpu.CompilerParams(vmem_limit_bytes=60 * 2**20),
    )(total, upper_by, gated_by)
    gathered = lax.all_gather(both, "gy", axis=0)
    spread = pl.pallas_call(
        spread_kernel,
        in_specs=[pl.BlockSpec(memory_space=pltpu.SMEM), vmem, vmem, pl.BlockSpec(memory_space=pl.ANY)]
        + [vmem] * planes,
        out_shape=sds((slots, hidden), BF16),
        scratch_shapes=[pltpu.VMEM((hidden, tops * tokens), BF16)],
        cost_estimate=pl.CostEstimate(
            flops=2 * slots * hidden * tops * tokens, bytes_accessed=8 * slots * hidden, transcendentals=0
        ),
        compiler_params=pltpu.CompilerParams(vmem_limit_bytes=60 * 2**20),
    )(z.reshape(1), key, ids, both, *act_pieces)
    rows_hidden = lax.all_to_all(spread.reshape(experts, MOST, -1), GX, 0, 0, tiled=True)
    down_t = lax.dot_general(
        rows_kept, rows_hidden.reshape(slots, hidden), (((0,), (0,)), ((), ())), preferred_element_type=F32
    )
    grad_gate, grad_up = final_grads(act_turned, gathered)
    return (grad_gate[None], grad_up[None], down_t.astype(BF16).T[None])


def solution(mesh):
    torus = Mesh(mesh.devices.reshape(4, 4, 2, mesh.shape["gy"]), ("gx_0", "gx_1", "gx_2", "gy"))
    return jax.shard_map(
        on_device,
        mesh=torus,
        in_specs=(
            P(GX, "gy"),
            P(GX, "gy"),
            P(GX, None, "gy"),
            P(GX, None, "gy"),
            P(GX, None),
            P(GX, None),
            P(GX, None, "gy"),
        ),
        out_specs=(P(GX, "gy", None), P(GX, "gy", None), P(GX, None, "gy")),
        check_vma=False,
    )
```
